128 devices in a mesh: gx: 8 (over y, core), gy: 16 (over z, x).
Axes of the slice: x: 4, y: 4, z: 4, core: 2. Of those that a mesh axis runs over, the one named last changes fastest.
Arguments:
- basis: float32 [3, 400, 8, 20480], P(None, None, 'gx', 'gy'), may hold values from -0.3125 to 0.3125
- connectivity: int32 [8, 8, 16384], P(None, 'gx', 'gy'), may hold values from 0 to 1791
- send_nodes: int32 [4, 8, 2048], P(None, 'gx', 'gy'), may hold values from 0 to 1279
- modulus: float32 [8, 16384], P('gx', 'gy'), may hold values from 0.2 to 5
- ecsw_weight: float32 [8, 16384], P('gx', 'gy'), may hold values from 0.3 to 6
- stiffness: float32 [24, 24], replicated, may hold values from -1.25 to 1.25
- coords: float32 [400], replicated, may hold values from -6 to 6
- velocity: float32 [400], replicated, may hold values from -3 to 3
- external: float32 [400], replicated, may hold values from -12 to 12
Outputs:
- final_coords: float32 [400], replicated
- final_velocity: float32 [400], replicated
- reduced_force: float32 [400], replicated
- displaced: float32 [3, 8, 20480], P(None, 'gx', 'gy')
The draws below stay inside these ranges and needn't reach their ends.
Inputs may be any that keep to these rules, and one draw needn't show every extreme that they name: `connectivity`: entries index a partition's node table: its 1280 owned nodes, then 128 nodes from each of the neighbours below and above along gx, then below and above along gy. `send_nodes`: Owned-node indices of a partition, 128 for each neighbour, in the order below and above along gx, below and above along gy; an index may repeat.
All inputs are finite; a program needn't handle non-finite values.
Results may differ from the reference program's by a relative error of at most 0.0003.
Values sent between devices are 32-bit elements; how exact they have to be, the bound alone decides.
No kernel may reach another device: no remote copies, remote signals or barrier semaphores. Data moves between devices by JAX's collectives and lax.ppermute only.
A program may use at most 128 MiB of HBM per device.

```python
import math
import jax
import jax.numpy as jnp
from jax import lax

K = 400
NODES_DEV = 1280
ELEM_DEV = 1024
HALO = 128
STEPS = 2
SLOTS = 1792
ELEMENTS = 16384
NODES = 20480
N_GX = 8
N_GY = 16


def set_ends(drawn, rng, least, largest):
    longest = drawn.shape.index(max(drawn.shape))
    spots = []
    for shift in (0, 1):
        where = [jax.random.randint(jax.random.fold_in(rng, axis), (), 0, length) for axis, length in enumerate(drawn.shape)]
        where[longest] = (where[longest] + shift) % drawn.shape[longest]
        spots.append(tuple(where))
    return drawn.at[spots[0]].set(least).at[spots[1]].set(largest)


def block_levels(stream_key, shape, shards, least, high):
    loudness = 1.0
    for position, blocks in shards:
        heights = jax.random.uniform(jax.random.fold_in(jax.random.fold_in(stream_key, 6), position), (blocks,), jnp.float32, least / len(shards), high / len(shards))
        loudness = loudness * jnp.repeat(jnp.exp(heights), shape[position] // blocks).reshape((-1,) + (1,) * (len(shape) - 1 - position))
    return loudness


def gaussian(own_key, shape, scale, most, split=(), dtype=jnp.bfloat16):
    drawn = scale * jax.random.normal(own_key, shape, jnp.float32)
    if split:
        drawn = drawn * block_levels(own_key, shape, split, -0.22, 0.18)
    return jnp.clip(drawn, -most, most).astype(dtype)


def setup_inputs(seed: int = 0) -> dict:
    keys = jax.random.split(jax.random.key(seed), 10)
    return {
        "basis": gaussian(keys[0], (3, K, N_GX, NODES), K ** -0.5, 0.3125, ((2, 8), (3, 16)), jnp.float32),
        "connectivity": set_ends(jax.random.randint(keys[1], (8, N_GX, ELEMENTS), 0, SLOTS), jax.random.fold_in(keys[1], 1), 0, SLOTS - 1).astype(jnp.int32),
        "send_nodes": set_ends(jax.random.randint(keys[2], (4, N_GX, N_GY * HALO), 0, NODES_DEV), jax.random.fold_in(keys[2], 1), 0, NODES_DEV - 1).astype(jnp.int32),
        "modulus": jnp.clip(jnp.exp(math.log(5.0) - 3.218876 * jax.random.uniform(keys[3], (N_GX, ELEMENTS), jnp.float32) ** block_levels(keys[3], (N_GX, ELEMENTS), ((0, 8), (1, 16)), -0.2, 0.2)), 0.2, 5.0),
        "ecsw_weight": jnp.clip(jnp.exp(math.log(6.0) - 2.9957322 * jax.random.uniform(keys[4], (N_GX, ELEMENTS), jnp.float32) ** block_levels(keys[4], (N_GX, ELEMENTS), ((0, 8), (1, 16)), -0.2, 0.2)), 0.3, 6.0),
        "stiffness": gaussian(keys[5], (24, 24), 24 ** -0.5, 1.25, (), jnp.float32),
        "coords": gaussian(keys[6], (K,), 1.0, 6.0, (), jnp.float32),
        "velocity": gaussian(keys[7], (K,), 0.5, 3.0, (), jnp.float32),
        "external": gaussian(keys[8], (K,), 2.0, 12.0, (), jnp.float32),
    }


time_step = 0.05


def lower(array, axis):
    widths = [(0, 0)] * array.ndim
    widths[axis] = (1, 0)
    return lax.slice_in_dim(jnp.pad(array, widths), 0, array.shape[axis], axis=axis)


def upper(array, axis):
    widths = [(0, 0)] * array.ndim
    widths[axis] = (0, 1)
    return lax.slice_in_dim(jnp.pad(array, widths), 1, array.shape[axis] + 1, axis=axis)


def element_forces(moved, links, stiffness, factor):
    corner = moved[:, links]
    stacked = corner.reshape(24, links.shape[1])
    strain = jnp.dot(stiffness, stacked, precision=lax.Precision.HIGHEST)
    forces = factor * (strain + strain * strain * strain / 3.0)
    return jnp.zeros_like(moved).at[:, links].add(forces.reshape(3, 8, links.shape[1]))


def add_back(owned, indices, values):
    return owned.at[:, indices].add(values)


def reference(basis, connectivity, send_nodes, modulus, ecsw_weight, stiffness, coords, velocity, external):
    parts = N_GX * N_GY
    phi = basis.reshape(3, K, N_GX, N_GY, NODES_DEV)
    links = connectivity.reshape(8, parts, ELEM_DEV)
    senders = send_nodes.reshape(4, N_GX, N_GY, HALO)
    factor = (modulus * ecsw_weight).reshape(parts, ELEM_DEV)
    reduced = jnp.zeros_like(coords)
    for repeat in range(STEPS):
        moved = jnp.einsum("ckxyn,k->cxyn", phi, coords, precision=lax.Precision.HIGHEST)
        blocks = [jnp.take_along_axis(moved, jnp.broadcast_to(senders[side][None], (3, N_GX, N_GY, HALO)), axis=3) for side in range(4)]
        slots = [lower(blocks[1], 1), upper(blocks[0], 1), lower(blocks[3], 2), upper(blocks[2], 2)]
        lookup = jnp.concatenate([moved] + slots, axis=3).reshape(3, parts, SLOTS)
        nodal = jax.vmap(element_forces, in_axes=(1, 1, None, 0), out_axes=1)(lookup, links, stiffness, factor)
        nodal = nodal.reshape(3, N_GX, N_GY, SLOTS)
        margin = [nodal[..., NODES_DEV + side * HALO:NODES_DEV + (side + 1) * HALO] for side in range(4)]
        back = [lower(margin[1], 1), upper(margin[0], 1), lower(margin[3], 2), upper(margin[2], 2)]
        owned = nodal[..., :NODES_DEV].reshape(3, parts, NODES_DEV)
        for side in range(4):
            owned = jax.vmap(add_back, in_axes=(1, 0, 1), out_axes=1)(owned, senders[side].reshape(parts, HALO), back[side].reshape(3, parts, HALO))
        owned = owned.reshape(3, N_GX, N_GY, NODES_DEV)
        reduced = jnp.einsum("ckxyn,cxyn->k", phi, owned, precision=lax.Precision.HIGHEST)
        velocity = velocity + time_step * (external - reduced)
        coords = coords + time_step * velocity
    displaced = jnp.einsum("ckxyn,k->cxyn", phi, coords, precision=lax.Precision.HIGHEST)
    return coords, velocity, reduced, displaced.reshape(3, N_GX, N_GY * NODES_DEV)
```

```python
import functools

import jax
import jax.numpy as jnp
from jax import lax
from jax.experimental import pallas as pl
from jax.experimental.pallas import tpu as pltpu
from jax.sharding import PartitionSpec as P

STEPS = 2
DT = 0.05
LANES = 128
SPLITS = 3


def lane_pick(rows, lanes):
    return jnp.take_along_axis(rows, lanes, axis=1, mode="promise_in_bounds")


def load_chunks(basis_ref, buf, sems, chunks):
    size = buf.shape[0] // chunks
    copies = []
    for i in range(chunks):
        part = pl.ds(i * size, size)
        copies.append(pltpu.make_async_copy(basis_ref.at[part], buf.at[part], sems.at[i]))
    for copy in copies:
        copy.start()
    return copies


def shared_rows_kernel(modes, tiles, chunks, basis_ref, send_ref, first_ref, second_ref, buf, sems):
    copies = load_chunks(basis_ref, buf, sems, chunks)
    outs = (first_ref, second_ref)
    picks = []
    for side in range(2):
        nodes = jnp.broadcast_to(send_ref[side : side + 1, :], (8, LANES))
        picks.append((nodes & (LANES - 1), nodes >> 7))
    groups = first_ref.shape[0] // 8 // chunks
    for i in range(chunks):
        copies[i].wait()

        def body(g, carry, i=i):
            g = g + i * groups
            sums = [jnp.zeros((8, LANES), jnp.float32) for _ in range(2)]
            for t in range(tiles):
                rows = buf[pl.ds(g * (8 * tiles) + t, 8, stride=tiles), :]
                for side in range(2):
                    lanes, tile = picks[side]
                    sums[side] = jnp.where(tile == t, lane_pick(rows, lanes), sums[side])
            for side in range(2):
                outs[side][pl.ds(pl.multiple_of(g * 8, 8), 8), :] = sums[side]
            return carry

        lax.fori_loop(0, groups, body, 0, unroll=5)


def shared_rows(basis, send, modes):
    rows = basis.shape[0]
    comps = 3
    tiles = rows // (comps * modes)
    chunks = 6
    out = jax.ShapeDtypeStruct((comps * modes, LANES), jnp.float32)
    return pl.pallas_call(
        functools.partial(shared_rows_kernel, modes, tiles, chunks),
        out_shape=(out, out),
        in_specs=[pl.BlockSpec(memory_space=pl.ANY), pl.BlockSpec(memory_space=pltpu.VMEM)],
        out_specs=(pl.BlockSpec(memory_space=pltpu.VMEM),) * 2,
        scratch_shapes=[
            pltpu.VMEM((rows, LANES), jnp.float32),
            pltpu.SemaphoreType.DMA((chunks,)),
        ],
        compiler_params=pltpu.CompilerParams(vmem_limit_bytes=16 * 2**20),
        name="shared_rows",
    )(basis, send)


def newest(first, parts_ref, coords_ref, velocity_ref, external_ref):
    coords = coords_ref[...]
    velocity = velocity_ref[...]
    if first:
        return coords, velocity, None
    reduced = jnp.sum(parts_ref[...], axis=0, keepdims=True)
    velocity = velocity + DT * (external_ref[...] - reduced)
    coords = coords + DT * velocity
    return coords, velocity, reduced


def column(row):
    return jnp.transpose(jnp.broadcast_to(row, (LANES, row.shape[1])))


def contract(buf, cols, modes, tiles, comp):
    def body(k, sums):
        scale = cols[pl.ds(pl.multiple_of(k * 8, 8), 8), :]
        base = comp * modes * tiles + k * 8 * tiles
        return tuple(
            sums[t] + buf[pl.ds(base + t, 8, stride=tiles), :] * scale for t in range(tiles)
        )

    zero = jnp.zeros((8, LANES), jnp.float32)
    sums = lax.fori_loop(0, modes // 8, body, (zero,) * tiles, unroll=5)
    return [jnp.sum(s, axis=0, keepdims=True) for s in sums]


def contract_shared(sides, cols, modes, comp):
    def body(k, sums):
        scale = cols[pl.ds(pl.multiple_of(k * 8, 8), 8), :]
        start = pl.multiple_of(comp * modes + k * 8, 8)
        return tuple(s + side[pl.ds(start, 8), :] * scale for s, side in zip(sums, sides))

    zero = jnp.zeros((8, LANES), jnp.float32)
    sums = lax.fori_loop(0, modes // 8, body, (zero,) * len(sides), unroll=5)
    return [jnp.sum(s, axis=0, keepdims=True) for s in sums]


def step_kernel(first, modes, tiles, chunks, *refs):
    if first:
        (basis_ref, r0, r1, r2, r3, links_ref, modulus_ref, weight_ref, stiff_ref,
         coords_ref, velocity_ref, external_ref, out_ref,
         buf, sems, cols, table, corner, spread, low, nodal_ref, acc_ref) = refs
        parts_ref = None
    else:
        (parts_ref, basis_ref, r0, r1, r2, r3, links_ref, modulus_ref, weight_ref, stiff_ref,
         coords_ref, velocity_ref, external_ref, out_ref, coords_out, velocity_out,
         buf, sems, cols, table, corner, spread, low, nodal_ref, acc_ref) = refs
    sides = (r0, r1, r2, r3)
    slots = tiles + len(sides)
    copies = load_chunks(basis_ref, buf, sems, chunks)
    elements = links_ref.shape[1]
    blocks = elements // LANES

    iota = lax.broadcasted_iota(jnp.int32, (LANES, LANES), 0)
    for b in range(blocks):
        for a in range(8):
            links = links_ref[a : a + 1, b * LANES : (b + 1) * LANES]
            hot = jnp.broadcast_to(links & (LANES - 1), (LANES, LANES)) == iota
            at = a * elements + b * LANES
            low[:, at : at + LANES] = jnp.where(hot, 1.0, 0.0).astype(jnp.bfloat16)

    coords, velocity, _ = newest(first, parts_ref, coords_ref, velocity_ref, external_ref)
    if not first:
        coords_out[...] = coords
        velocity_out[...] = velocity
    cols[...] = column(coords)

    per = chunks // 3
    for c in range(3):
        for i in range(per):
            copies[c * per + i].wait()
        rows = contract(buf, cols, modes, tiles, c) + contract_shared(sides, cols, modes, c)
        for r, row in enumerate(rows):
            table[c * slots + r : c * slots + r + 1, :] = row

    for b in range(blocks):
        links = links_ref[:, b * LANES : (b + 1) * LANES]
        lanes, tile = links & (LANES - 1), links >> 7
        for c in range(3):
            value = jnp.zeros((8, LANES), jnp.float32)
            for r in range(slots):
                row = jnp.broadcast_to(table[c * slots + r : c * slots + r + 1, :], (8, LANES))
                value = jnp.where(tile == r, lane_pick(row, lanes), value)
            corner[c * 8 : (c + 1) * 8, b * LANES : (b + 1) * LANES] = value

    strain = jnp.dot(
        stiff_ref[...], corner[...],
        precision=lax.Precision.HIGHEST, preferred_element_type=jnp.float32,
    )
    factor = modulus_ref[...] * weight_ref[...]
    corner[...] = factor * (strain + strain * strain * strain * (1.0 / 3.0))

    high = lax.broadcasted_iota(jnp.int32, (16, LANES), 0)
    for b in range(blocks):
        part = slice(b * LANES, (b + 1) * LANES)
        pieces = []
        rest = corner[:, part]
        for s in range(SPLITS):
            piece = rest.astype(jnp.bfloat16).astype(jnp.float32)
            pieces.append(piece)
            rest = rest - piece
        for a in range(8):
            hot = jnp.broadcast_to(links_ref[a : a + 1, part] >> 7, (16, LANES)) == high
            at = a * elements + b * LANES
            for s in range(SPLITS):
                for c in range(3):
                    row = c * 8 + a
                    value = jnp.broadcast_to(pieces[s][row : row + 1, :], (16, LANES))
                    to = (s * 3 + c) * 16
                    spread[to : to + 16, at : at + LANES] = jnp.where(hot, value, 0.0).astype(
                        jnp.bfloat16
                    )
    nodal = lax.dot_general(
        spread[...], low[...], (((1,), (1,)), ((), ())), preferred_element_type=jnp.float32
    )
    total = nodal[0:48]
    for s in range(1, SPLITS):
        total = total + nodal[s * 48 : (s + 1) * 48]
    nodal_ref[...] = total

    def body(k, carry):
        for j in range(2):
            g = k * 2 + j
            value = jnp.zeros((8, LANES), jnp.float32)
            for c in range(3):
                base = c * modes * tiles + g * 8 * tiles
                for r in range(slots):
                    row = jnp.broadcast_to(nodal_ref[c * 16 + r : c * 16 + r + 1, :], (8, LANES))
                    if r < tiles:
                        rows = buf[pl.ds(base + r, 8, stride=tiles), :]
                    else:
                        rows = sides[r - tiles][pl.ds(pl.multiple_of(c * modes + g * 8, 8), 8), :]
                    value = value + rows * row
            acc_ref[pl.ds(pl.multiple_of(g * 8, 8), 8), :] = value
        return carry

    lax.fori_loop(0, modes // 16, body, 0)
    sums = jnp.sum(jnp.transpose(acc_ref[...]), axis=0, keepdims=True)
    out_ref[...] = jnp.broadcast_to(sums, out_ref.shape)


def final_kernel(modes, tiles, chunks, parts_ref, basis_ref, coords_ref, velocity_ref, external_ref,
                 coords_out, velocity_out, reduced_out, displaced_out, buf, sems, cols):
    copies = load_chunks(basis_ref, buf, sems, chunks)
    coords, velocity, reduced = newest(False, parts_ref, coords_ref, velocity_ref, external_ref)
    coords_out[...] = coords
    velocity_out[...] = velocity
    reduced_out[...] = reduced
    cols[...] = column(coords)
    per = chunks // 3
    for c in range(3):
        for i in range(per):
            copies[c * per + i].wait()
        for r, row in enumerate(contract(buf, cols, modes, tiles, c)):
            displaced_out[c * tiles + r : c * tiles + r + 1, :] = row


VMEM = pl.BlockSpec(memory_space=pltpu.VMEM)
ANY = pl.BlockSpec(memory_space=pl.ANY)


def step(first, parts, basis, sides, links, modulus, weight, stiffness, coords, velocity, external, devices):
    modes = coords.shape[1]
    tiles = basis.shape[0] // (3 * modes)
    chunks = 6
    elements = links.shape[1]
    slots = tiles + 4
    vector = jax.ShapeDtypeStruct((1, modes), jnp.float32)
    outs = [jax.ShapeDtypeStruct((devices, modes), jnp.float32)]
    args = [basis, *sides, links, modulus, weight, stiffness, coords, velocity, external]
    specs = [ANY] + [VMEM] * (len(args) - 1)
    if not first:
        args = [parts] + args
        specs = [VMEM] + specs
        outs += [vector, vector]
    return pl.pallas_call(
        functools.partial(step_kernel, first, modes, tiles, chunks),
        out_shape=tuple(outs),
        in_specs=specs,
        out_specs=(VMEM,) * len(outs),
        scratch_shapes=[
            pltpu.VMEM(basis.shape, jnp.float32),
            pltpu.SemaphoreType.DMA((chunks,)),
            pltpu.VMEM((modes, LANES), jnp.float32),
            pltpu.VMEM((-(-3 * slots // 8) * 8, LANES), jnp.float32),
            pltpu.VMEM((24, elements), jnp.float32),
            pltpu.VMEM((SPLITS * 48, 8 * elements), jnp.bfloat16),
            pltpu.VMEM((LANES, 8 * elements), jnp.bfloat16),
            pltpu.VMEM((48, LANES), jnp.float32),
            pltpu.VMEM((modes, LANES), jnp.float32),
        ],
        compiler_params=pltpu.CompilerParams(vmem_limit_bytes=32 * 2**20),
        name="first_step" if first else "next_step",
    )(*args)


def finish(parts, basis, coords, velocity, external):
    modes = coords.shape[1]
    tiles = basis.shape[0] // (3 * modes)
    chunks = 6
    vector = jax.ShapeDtypeStruct((1, modes), jnp.float32)
    return pl.pallas_call(
        functools.partial(final_kernel, modes, tiles, chunks),
        out_shape=(vector, vector, vector, jax.ShapeDtypeStruct((3 * tiles, LANES), jnp.float32)),
        in_specs=[VMEM, ANY, VMEM, VMEM, VMEM],
        out_specs=(VMEM,) * 4,
        scratch_shapes=[
            pltpu.VMEM(basis.shape, jnp.float32),
            pltpu.SemaphoreType.DMA((chunks,)),
            pltpu.VMEM((modes, LANES), jnp.float32),
        ],
        compiler_params=pltpu.CompilerParams(vmem_limit_bytes=16 * 2**20),
        name="finish",
    )(parts, basis, coords, velocity, external)


def shards(basis, connectivity, send_nodes, modulus, ecsw_weight, stiffness, coords, velocity, external):
    modes = coords.shape[0]
    nodes = basis.shape[3]
    flat = basis.reshape(3 * modes * nodes // LANES, LANES)
    links = connectivity[:, 0, :]
    senders = send_nodes[:, 0, :]
    coords, velocity, external = (x[None, :] for x in (coords, velocity, external))

    below_y, above_y = shared_rows(flat, senders[2:4], modes)
    n_y = lax.axis_size("gy")
    up_y = [(i, i + 1) for i in range(n_y - 1)]
    down_y = [(j, i) for i, j in up_y]
    r2 = lax.ppermute(above_y, "gy", up_y)
    r3 = lax.ppermute(below_y, "gy", down_y)
    below_x, above_x = shared_rows(flat, senders[0:2], modes)
    n_x = lax.axis_size("gx")
    up_x = [(i, i + 1) for i in range(n_x - 1)]
    down_x = [(j, i) for i, j in up_x]
    r0 = lax.ppermute(above_x, "gx", up_x)
    r1 = lax.ppermute(below_x, "gx", down_x)
    sides = (r0, r1, r2, r3)

    devices = n_x * n_y
    both = ("gx", "gy")
    (parts,) = step(True, None, flat, sides, links, modulus, ecsw_weight, stiffness, coords, velocity, external, devices)
    for _ in range(STEPS - 1):
        parts = lax.all_to_all(parts, both, 0, 0, tiled=True)
        parts, coords, velocity = step(
            False, parts, flat, sides, links, modulus, ecsw_weight, stiffness, coords, velocity, external, devices
        )
    parts = lax.all_to_all(parts, both, 0, 0, tiled=True)
    coords, velocity, reduced, displaced = finish(parts, flat, coords, velocity, external)
    return coords[0], velocity[0], reduced[0], displaced.reshape(3, 1, nodes)


def solution(mesh):
    return jax.shard_map(
        shards,
        mesh=mesh,
        in_specs=(
            P(None, None, "gx", "gy"),
            P(None, "gx", "gy"),
            P(None, "gx", "gy"),
            P("gx", "gy"),
            P("gx", "gy"),
            P(),
            P(),
            P(),
            P(),
        ),
        out_specs=(P(), P(), P(), P(None, "gx", "gy")),
        check_vma=False,
    )
```

```python
import functools

import jax
import jax.numpy as jnp
from jax import lax
from jax.experimental import pallas as pl
from jax.experimental.pallas import tpu as pltpu
from jax.sharding import PartitionSpec as P

STEPS = 2
DT = 0.05
LANES = 128
SPLITS = 3
MIB = 2**20

VMEM = pl.BlockSpec(memory_space=pltpu.VMEM)
HBM = pl.BlockSpec(memory_space=pltpu.HBM)


def lane_pick(rows, lanes):
    return jnp.take_along_axis(rows, lanes, axis=1, mode="promise_in_bounds")


def eight(start):
    return pl.ds(pl.multiple_of(start, 8), 8)


def picks_of(send_ref, sides):
    picks = []
    for side in sides:
        nodes = jnp.broadcast_to(send_ref[side], (8, LANES))
        picks.append((nodes & (LANES - 1), nodes >> 7))
    return picks


def pick_rows(tiles, picks):
    sums = [jnp.zeros((8, LANES), jnp.float32) for _ in picks]
    for t, rows in enumerate(tiles):
        for side, (lanes, tile) in enumerate(picks):
            sums[side] = jnp.where(tile == t, lane_pick(rows, lanes), sums[side])
    return sums


def load_kernel(modes, tiles, chunks, basis_ref, send_ref, dense_ref, below_ref, above_ref, buf, sems):
    size = buf.shape[0] // chunks
    copies = [
        pltpu.make_async_copy(
            basis_ref.at[pl.ds(i * size, size)], buf.at[pl.ds(i * size, size)], sems.at[i]
        )
        for i in range(chunks)
    ]
    for copy in copies:
        copy.start()
    picks = picks_of(send_ref, (2, 3))
    groups = size // (8 * tiles)
    per = chunks // 3
    for i in range(chunks):
        comp = i // per
        copies[i].wait()

        def body(g, carry, i=i, comp=comp):
            mode = (g + (i % per) * groups) * 8
            row = (g + i * groups) * (8 * tiles)
            read = []
            for t in range(tiles):
                rows = buf[pl.ds(row + t, 8, stride=tiles), :]
                dense_ref[eight((comp * tiles + t) * modes + mode), :] = rows
                read.append(rows)
            for ref, value in zip((below_ref, above_ref), pick_rows(read, picks)):
                ref[eight(comp * modes + mode), :] = value
            return carry

        lax.fori_loop(0, groups, body, 0, unroll=25)


def load(basis, send, modes):
    rows = basis.shape[0]
    tiles = rows // (3 * modes)
    chunks = 6
    shared = jax.ShapeDtypeStruct((3 * modes, LANES), jnp.float32)
    return pl.pallas_call(
        functools.partial(load_kernel, modes, tiles, chunks),
        out_shape=(jax.ShapeDtypeStruct(basis.shape, jnp.float32), shared, shared),
        in_specs=[HBM, VMEM],
        out_specs=(VMEM,) * 3,
        scratch_shapes=[
            pltpu.VMEM((rows, LANES), jnp.float32),
            pltpu.SemaphoreType.DMA((chunks,)),
        ],
        compiler_params=pltpu.CompilerParams(vmem_limit_bytes=24 * MIB),
        name="load",
    )(basis, send)


def share_kernel(modes, tiles, dense_ref, send_ref, below_ref, above_ref):
    picks = picks_of(send_ref, (0, 1))

    for c in range(3):

        def body(g, carry, c=c):
            read = [dense_ref[eight((c * tiles + t) * modes + g * 8), :] for t in range(tiles)]
            for ref, value in zip((below_ref, above_ref), pick_rows(read, picks)):
                ref[eight(c * modes + g * 8), :] = value
            return carry

        lax.fori_loop(0, modes // 8, body, 0, unroll=25)


def share(dense, send, modes):
    tiles = dense.shape[0] // (3 * modes)
    shared = jax.ShapeDtypeStruct((3 * modes, LANES), jnp.float32)
    return pl.pallas_call(
        functools.partial(share_kernel, modes, tiles),
        out_shape=(shared, shared),
        in_specs=[VMEM, VMEM],
        out_specs=(VMEM,) * 2,
        compiler_params=pltpu.CompilerParams(vmem_limit_bytes=16 * MIB),
        name="share",
    )(dense, send)


def column(row):
    return jnp.transpose(jnp.broadcast_to(row, (LANES, row.shape[1])))


def contract(places, cols, modes):
    def body(k, sums):
        scale = cols[eight(k * 8), :]
        return tuple(s + ref[eight(at + k * 8), :] * scale for s, (ref, at) in zip(sums, places))

    zero = jnp.zeros((8, LANES), jnp.float32)
    sums = lax.fori_loop(0, modes // 8, body, (zero,) * len(places), unroll=2)
    return [jnp.sum(s, axis=0, keepdims=True) for s in sums]


def owned_places(dense_ref, modes, tiles):
    return [(dense_ref, (c * tiles + t) * modes) for c in range(3) for t in range(tiles)]


def shared_places(sides, modes):
    return [(side, c * modes) for c in range(3) for side in sides]


def prepare_kernel(modes, tiles, dense_ref, links_ref, coords_ref, owned_ref, low_ref, high_ref, cols):
    cols[...] = column(coords_ref[...])
    for i, row in enumerate(contract(owned_places(dense_ref, modes, tiles), cols, modes)):
        owned_ref[i : i + 1, :] = row
    elements = links_ref.shape[1]
    for b in range(elements // LANES):
        for a in range(8):
            links = links_ref[a : a + 1, b * LANES : (b + 1) * LANES]
            at = slice(a * elements + b * LANES, a * elements + (b + 1) * LANES)
            for ref, bits, size in ((low_ref, links & (LANES - 1), LANES), (high_ref, links >> 7, 16)):
                count = lax.broadcasted_iota(jnp.int32, (size, LANES), 0)
                hot = jnp.broadcast_to(bits, (size, LANES)) == count
                ref[:, at] = jnp.where(hot, 1.0, 0.0).astype(jnp.bfloat16)


def prepare(dense, links, coords):
    modes = coords.shape[1]
    tiles = dense.shape[0] // (3 * modes)
    entries = 8 * links.shape[1]
    return pl.pallas_call(
        functools.partial(prepare_kernel, modes, tiles),
        out_shape=(
            jax.ShapeDtypeStruct((-(-3 * tiles // 8) * 8, LANES), jnp.float32),
            jax.ShapeDtypeStruct((LANES, entries), jnp.bfloat16),
            jax.ShapeDtypeStruct((16, entries), jnp.bfloat16),
        ),
        in_specs=[VMEM] * 3,
        out_specs=(VMEM,) * 3,
        scratch_shapes=[pltpu.VMEM((modes, LANES), jnp.float32)],
        compiler_params=pltpu.CompilerParams(vmem_limit_bytes=16 * MIB),
        name="prepare",
    )(dense, links, coords)


def advance(parts_ref, coords_ref, velocity_ref, external_ref):
    sums = jnp.sum(parts_ref[...].reshape(-1, 8, LANES), axis=0)
    pair = sums[0:4] + sums[4:8]
    modes = coords_ref.shape[1]
    reduced = jnp.concatenate([pair[r : r + 1] for r in range(4)], axis=1)[:, :modes]
    velocity = velocity_ref[...] + DT * (external_ref[...] - reduced)
    coords = coords_ref[...] + DT * velocity
    return coords, velocity, reduced


def step_kernel(first, modes, tiles, *refs):
    if first:
        (owned_ref, dense_ref, r0, r1, r2, r3, links_ref, low_ref, high_ref, modulus_ref, weight_ref, stiff_ref,
         coords_ref, out_ref, cols, table, corner, pieces, spread) = refs
        coords = coords_ref[...]
    else:
        (parts_ref, dense_ref, r0, r1, r2, r3, links_ref, low_ref, high_ref, modulus_ref, weight_ref, stiff_ref,
         coords_ref, velocity_ref, external_ref, out_ref, coords_out, velocity_out,
         cols, table, corner, pieces, spread) = refs
        coords, velocity, _ = advance(parts_ref, coords_ref, velocity_ref, external_ref)
        coords_out[...] = coords
        velocity_out[...] = velocity
    sides = (r0, r1, r2, r3)
    slots = tiles + 4
    elements = links_ref.shape[1]
    blocks = elements // LANES

    cols[...] = column(coords)
    if first:
        owned = [owned_ref[i : i + 1, :] for i in range(3 * tiles)]
        shared = contract(shared_places(sides, modes), cols, modes)
    else:
        rows = contract(
            owned_places(dense_ref, modes, tiles) + shared_places(sides, modes), cols, modes
        )
        owned, shared = rows[: 3 * tiles], rows[3 * tiles :]
    for c in range(3):
        rows = owned[c * tiles : (c + 1) * tiles] + shared[c * 4 : (c + 1) * 4]
        for r, row in enumerate(rows):
            table[c * slots + r : c * slots + r + 1, :] = row

    for b in range(blocks):
        links = links_ref[:, b * LANES : (b + 1) * LANES]
        lanes, tile = links & (LANES - 1), links >> 7
        for c in range(3):
            value = jnp.zeros((8, LANES), jnp.float32)
            for r in range(slots):
                row = jnp.broadcast_to(table[c * slots + r : c * slots + r + 1, :], (8, LANES))
                value = jnp.where(tile == r, lane_pick(row, lanes), value)
            corner[c * 8 : (c + 1) * 8, b * LANES : (b + 1) * LANES] = value

    strain = jnp.dot(
        stiff_ref[...], corner[...],
        precision=lax.Precision.HIGHEST, preferred_element_type=jnp.float32,
    )
    factor = modulus_ref[...] * weight_ref[...]
    rest = factor * (strain + strain * strain * strain * (1.0 / 3.0))
    for s in range(SPLITS):
        piece = rest.astype(jnp.bfloat16).astype(jnp.float32)
        pieces[s * 24 : (s + 1) * 24, :] = piece
        rest = rest - piece

    for b in range(blocks):
        part = slice(b * LANES, (b + 1) * LANES)
        for a in range(8):
            at = slice(a * elements + b * LANES, a * elements + (b + 1) * LANES)
            hot = high_ref[:, at]
            for g in range(SPLITS * 3):
                row = pieces[g * 8 + a : g * 8 + a + 1, part]
                value = jnp.broadcast_to(row, (16, LANES)).astype(jnp.bfloat16)
                spread[g * 16 : (g + 1) * 16, at] = hot * value
    nodal = lax.dot_general(
        spread[...], low_ref[...], (((1,), (1,)), ((), ())), preferred_element_type=jnp.float32
    )
    total = nodal[0:48]
    for s in range(1, SPLITS):
        total = total + nodal[s * 48 : (s + 1) * 48]

    places = []
    for c in range(3):
        for r in range(slots):
            row = jnp.broadcast_to(total[c * 16 + r : c * 16 + r + 1], (8, LANES))
            if r < tiles:
                places.append((dense_ref, (c * tiles + r) * modes, row))
            else:
                places.append((sides[r - tiles], c * modes, row))

    def body(k, carry):
        sums = [jnp.zeros((8, LANES), jnp.float32) for _ in range(3)]
        for i, (ref, at, row) in enumerate(places):
            sums[i % 3] = sums[i % 3] + ref[eight(at + k * 8), :] * row
        cols[eight(k * 8), :] = sums[0] + sums[1] + sums[2]
        return carry

    lax.fori_loop(0, modes // 8, body, 0, unroll=2)
    sums = jnp.sum(jnp.transpose(cols[...]), axis=0, keepdims=True)
    sums = jnp.concatenate([sums, jnp.zeros((1, 4 * LANES - modes), jnp.float32)], axis=1)
    pair = [sums[:, r * LANES : (r + 1) * LANES] for r in range(4)]
    pair = jnp.concatenate(pair + pair, axis=0)
    out_ref[...] = jnp.broadcast_to(pair[None], (out_ref.shape[0] // 8, 8, LANES)).reshape(out_ref.shape)


def step(first, parts, dense, sides, links, low, high, modulus, weight, stiffness, vectors, devices):
    modes = vectors[0].shape[1]
    tiles = dense.shape[0] // (3 * modes)
    elements = links.shape[1]
    slots = tiles + 4
    vector = jax.ShapeDtypeStruct((1, modes), jnp.float32)
    outs = [jax.ShapeDtypeStruct((devices * 4, LANES), jnp.float32)]
    args = [parts, dense, *sides, links, low, high, modulus, weight, stiffness]
    if first:
        args += vectors[:1]
    else:
        args += vectors
        outs += [vector, vector]
    return pl.pallas_call(
        functools.partial(step_kernel, first, modes, tiles),
        out_shape=tuple(outs),
        in_specs=[VMEM] * len(args),
        out_specs=(VMEM,) * len(outs),
        scratch_shapes=[
            pltpu.VMEM((modes, LANES), jnp.float32),
            pltpu.VMEM((-(-3 * slots // 8) * 8, LANES), jnp.float32),
            pltpu.VMEM((24, elements), jnp.float32),
            pltpu.VMEM((SPLITS * 24, elements), jnp.float32),
            pltpu.VMEM((SPLITS * 48, 8 * elements), jnp.bfloat16),
        ],
        compiler_params=pltpu.CompilerParams(vmem_limit_bytes=24 * MIB),
        name="first_step" if first else "next_step",
    )(*args)


def final_kernel(modes, tiles, parts_ref, dense_ref, coords_ref, velocity_ref, external_ref,
                 coords_out, velocity_out, reduced_out, displaced_out, cols):
    coords, velocity, reduced = advance(parts_ref, coords_ref, velocity_ref, external_ref)
    coords_out[...] = coords
    velocity_out[...] = velocity
    reduced_out[...] = reduced
    cols[...] = column(coords)
    for i, row in enumerate(contract(owned_places(dense_ref, modes, tiles), cols, modes)):
        c, t = divmod(i, tiles)
        displaced_out[c, :, t * LANES : (t + 1) * LANES] = row


def finish(parts, dense, vectors):
    modes = vectors[0].shape[1]
    tiles = dense.shape[0] // (3 * modes)
    vector = jax.ShapeDtypeStruct((1, modes), jnp.float32)
    return pl.pallas_call(
        functools.partial(final_kernel, modes, tiles),
        out_shape=(vector, vector, vector, jax.ShapeDtypeStruct((3, 1, tiles * LANES), jnp.float32)),
        in_specs=[VMEM] * 5,
        out_specs=(VMEM,) * 4,
        scratch_shapes=[pltpu.VMEM((modes, LANES), jnp.float32)],
        compiler_params=pltpu.CompilerParams(vmem_limit_bytes=16 * MIB),
        name="finish",
    )(parts, dense, *vectors)


def exchange(below, above, axis):
    count = lax.axis_size(axis)
    up = [(i, i + 1) for i in range(count - 1)]
    down = [(j, i) for i, j in up]
    return lax.ppermute(above, axis, up), lax.ppermute(below, axis, down)


def everyone(parts, devices):
    chunks = parts.reshape(devices, parts.shape[0] // devices, LANES)
    return lax.all_to_all(chunks, ("gx", "gy"), 0, 0, tiled=True).reshape(parts.shape)


def shards(basis, connectivity, send_nodes, modulus, ecsw_weight, stiffness, coords, velocity, external):
    modes = coords.shape[0]
    nodes = basis.shape[3]
    flat = basis.reshape(3 * modes * nodes // LANES, LANES)
    links = connectivity[:, 0, :]
    coords, velocity, external = (x[None, :] for x in (coords, velocity, external))
    devices = lax.axis_size("gx") * lax.axis_size("gy")

    flat = pltpu.with_memory_space_constraint(flat, pltpu.HBM)
    dense, below, above = load(flat, send_nodes, modes)
    r2, r3 = exchange(below, above, "gy")
    below, above = share(dense, send_nodes, modes)
    r0, r1 = exchange(below, above, "gx")
    owned, low, high = prepare(dense, links, coords)
    sides = (r0, r1, r2, r3)

    (parts,) = step(True, owned, dense, sides, links, low, high, modulus, ecsw_weight, stiffness, (coords,), devices)
    for _ in range(STEPS - 1):
        parts, coords, velocity = step(
            False, everyone(parts, devices), dense, sides, links, low, high, modulus, ecsw_weight, stiffness,
            (coords, velocity, external), devices,
        )
    coords, velocity, reduced, displaced = finish(everyone(parts, devices), dense, (coords, velocity, external))
    return coords[0], velocity[0], reduced[0], displaced


def solution(mesh):
    return jax.shard_map(
        shards,
        mesh=mesh,
        in_specs=(
            P(None, None, "gx", "gy"),
            P(None, "gx", "gy"),
            P(None, "gx", "gy"),
            P("gx", "gy"),
            P("gx", "gy"),
            P(),
            P(),
            P(),
            P(),
        ),
        out_specs=(P(), P(), P(), P(None, "gx", "gy")),
        check_vma=False,
    )
```

```python
import functools

import jax
import jax.numpy as jnp
from jax import lax
from jax.experimental import pallas as pl
from jax.experimental.pallas import tpu as pltpu
from jax.sharding import PartitionSpec as P

STEPS = 2
DT = 0.05
LANES = 128
SPLITS = 3
CHUNKS = 6
MIB = 2**20

VMEM = pl.BlockSpec(memory_space=pltpu.VMEM)
HBM = pl.BlockSpec(memory_space=pltpu.HBM)


def lane_pick(rows, lanes):
    return jnp.take_along_axis(rows, lanes, axis=1, mode="promise_in_bounds")


def eight(start):
    return pl.ds(pl.multiple_of(start, 8), 8)


def load_kernel(modes, tiles, chunks, basis_ref, send_hbm, dense_ref, *refs):
    outs, (buf, send_ref, hot_ref, sems, send_sem) = refs[:4], refs[4:]
    size = buf.shape[0] // chunks
    copies = [
        pltpu.make_async_copy(
            basis_ref.at[pl.ds(i * size, size)], buf.at[pl.ds(i * size, size)], sems.at[i]
        )
        for i in range(chunks)
    ]
    lists = pltpu.make_async_copy(send_hbm, send_ref, send_sem)
    lists.start()
    for copy in copies:
        copy.start()
    lists.wait()

    picks = []
    for side in range(2):
        nodes = jnp.broadcast_to(send_ref[side], (8, LANES))
        picks.append((nodes & (LANES - 1), nodes >> 7))
    for t in range(tiles):
        count = lax.broadcasted_iota(jnp.int32, (LANES, LANES), 0) + t * LANES
        for side in range(2):
            hot = jnp.broadcast_to(send_ref[2 + side], (LANES, LANES)) == count
            hot_ref[t * LANES : (t + 1) * LANES, side * LANES : (side + 1) * LANES] = jnp.where(
                hot, 1.0, 0.0
            ).astype(jnp.bfloat16)

    groups = size // (8 * tiles)
    per = chunks // 3
    for i in range(chunks):
        copies[i].wait()
        comp, first = i // per, (i % per) * groups * 8
        columns = []
        for t in range(tiles):
            parts = [buf[pl.ds((i * groups + g) * 8 * tiles + t, 8, stride=tiles), :] for g in range(groups)]
            columns.append(jnp.concatenate(parts, axis=0))
            at = (comp * tiles + t) * modes + first
            dense_ref[at : at + groups * 8, :] = columns[t]
        at = slice(comp * modes + first, comp * modes + first + groups * 8)
        for side, (lanes, tile) in enumerate(picks):
            for g in range(groups):
                value = jnp.zeros((8, LANES), jnp.float32)
                for t in range(tiles):
                    value = jnp.where(tile == t, lane_pick(columns[t][g * 8 : (g + 1) * 8], lanes), value)
                outs[side][at.start + g * 8 : at.start + (g + 1) * 8, :] = value
        whole = jnp.concatenate(columns, axis=1)
        half = 96
        for lo, hi in ((0, half), (half, groups * 8)):
            rest = whole[lo:hi]
            total = None
            for s in range(3):
                piece = rest.astype(jnp.bfloat16)
                rest = rest - piece.astype(jnp.float32)
                part = jnp.dot(piece, hot_ref[...], preferred_element_type=jnp.float32)
                total = part if total is None else total + part
            outs[2][at.start + lo : at.start + hi, :] = total[:, :LANES]
            outs[3][at.start + lo : at.start + hi, :] = total[:, LANES:]


def load(basis, send, modes):
    rows = basis.shape[0]
    tiles = rows // (3 * modes)
    chunks = CHUNKS
    shared = jax.ShapeDtypeStruct((3 * modes, LANES), jnp.float32)
    basis = pltpu.with_memory_space_constraint(basis, pltpu.HBM)
    send = pltpu.with_memory_space_constraint(send, pltpu.HBM)
    return pl.pallas_call(
        functools.partial(load_kernel, modes, tiles, chunks),
        out_shape=(jax.ShapeDtypeStruct(basis.shape, jnp.float32),) + (shared,) * 4,
        in_specs=[HBM, HBM],
        out_specs=(VMEM,) * 5,
        scratch_shapes=[
            pltpu.VMEM((rows, LANES), jnp.float32),
            pltpu.VMEM(send.shape, jnp.int32),
            pltpu.VMEM((tiles * LANES, 2 * LANES), jnp.bfloat16),
            pltpu.SemaphoreType.DMA((chunks,)),
            pltpu.SemaphoreType.DMA,
        ],
        compiler_params=pltpu.CompilerParams(vmem_limit_bytes=24 * MIB),
        name="load",
    )(basis, send)


def edges():
    x, y = lax.axis_index("gx"), lax.axis_index("gy")
    return x > 0, x < lax.axis_size("gx") - 1, y > 0, y < lax.axis_size("gy") - 1


def column(row):
    return jnp.transpose(jnp.broadcast_to(row, (LANES, row.shape[1])))


def contract(places, cols, modes):
    def body(k, sums):
        scale = cols[eight(k * 8), :]
        return tuple(s + ref[eight(at + k * 8), :] * scale for s, (ref, at) in zip(sums, places))

    zero = jnp.zeros((8, LANES), jnp.float32)
    sums = lax.fori_loop(0, modes // 8, body, (zero,) * len(places), unroll=2)
    return [jnp.sum(s, axis=0, keepdims=True) for s in sums]


def owned_places(dense_ref, modes, tiles):
    return [(dense_ref, (c * tiles + t) * modes) for c in range(3) for t in range(tiles)]


def shared_places(sides, modes):
    return [(side, c * modes) for c in range(3) for side in sides]


def prepare_kernel(modes, tiles, dense_ref, links_ref, coords_ref, owned_ref, low_ref, high_ref, cols):
    cols[...] = column(coords_ref[...])
    for i, row in enumerate(contract(owned_places(dense_ref, modes, tiles), cols, modes)):
        owned_ref[i : i + 1, :] = row
    elements = links_ref.shape[1]
    for b in range(elements // LANES):
        for a in range(8):
            links = links_ref[a : a + 1, b * LANES : (b + 1) * LANES]
            at = slice(a * elements + b * LANES, a * elements + (b + 1) * LANES)
            for ref, bits, size in ((low_ref, links & (LANES - 1), LANES), (high_ref, links >> 7, 16)):
                count = lax.broadcasted_iota(jnp.int32, (size, LANES), 0)
                hot = jnp.broadcast_to(bits, (size, LANES)) == count
                ref[:, at] = jnp.where(hot, 1.0, 0.0).astype(jnp.bfloat16)


def prepare(dense, links, coords):
    modes = coords.shape[1]
    tiles = dense.shape[0] // (3 * modes)
    entries = 8 * links.shape[1]
    return pl.pallas_call(
        functools.partial(prepare_kernel, modes, tiles),
        out_shape=(
            jax.ShapeDtypeStruct((-(-3 * tiles // 8) * 8, LANES), jnp.float32),
            jax.ShapeDtypeStruct((LANES, entries), jnp.bfloat16),
            jax.ShapeDtypeStruct((16, entries), jnp.bfloat16),
        ),
        in_specs=[VMEM] * 3,
        out_specs=(VMEM,) * 3,
        scratch_shapes=[pltpu.VMEM((modes, LANES), jnp.float32)],
        compiler_params=pltpu.CompilerParams(vmem_limit_bytes=16 * MIB),
        name="prepare",
    )(dense, links, coords)


def advance(parts_ref, coords_ref, velocity_ref, external_ref):
    sums = jnp.sum(parts_ref[...].reshape(-1, 8, LANES), axis=0)
    pair = sums[0:4] + sums[4:8]
    modes = coords_ref.shape[1]
    reduced = jnp.concatenate([pair[r : r + 1] for r in range(4)], axis=1)[:, :modes]
    velocity = velocity_ref[...] + DT * (external_ref[...] - reduced)
    coords = coords_ref[...] + DT * velocity
    return coords, velocity, reduced


def step_kernel(first, modes, tiles, *refs):
    if first:
        (owned_ref, dense_ref, r0, r1, r2, r3, links_ref, low_ref, high_ref, modulus_ref, weight_ref, stiff_ref,
         coords_ref, out_ref, cols, table, corner, pieces, spread) = refs
        coords = coords_ref[...]
    else:
        (parts_ref, dense_ref, r0, r1, r2, r3, links_ref, low_ref, high_ref, modulus_ref, weight_ref, stiff_ref,
         coords_ref, velocity_ref, external_ref, out_ref, coords_out, velocity_out,
         cols, table, corner, pieces, spread) = refs
        coords, velocity, _ = advance(parts_ref, coords_ref, velocity_ref, external_ref)
        coords_out[...] = coords
        velocity_out[...] = velocity
    sides = (r0, r1, r2, r3)
    present = edges()
    slots = tiles + 4
    elements = links_ref.shape[1]
    blocks = elements // LANES

    cols[...] = column(coords)
    if first:
        owned = [owned_ref[i : i + 1, :] for i in range(3 * tiles)]
        shared = contract(shared_places(sides, modes), cols, modes)
    else:
        rows = contract(
            owned_places(dense_ref, modes, tiles) + shared_places(sides, modes), cols, modes
        )
        owned, shared = rows[: 3 * tiles], rows[3 * tiles :]
    for c in range(3):
        rows = owned[c * tiles : (c + 1) * tiles]
        rows += [jnp.where(here, row, 0.0) for here, row in zip(present, shared[c * 4 : (c + 1) * 4])]
        for r, row in enumerate(rows):
            table[c * slots + r : c * slots + r + 1, :] = row

    for b in range(blocks):
        links = links_ref[:, b * LANES : (b + 1) * LANES]
        lanes, tile = links & (LANES - 1), links >> 7
        for c in range(3):
            value = jnp.zeros((8, LANES), jnp.float32)
            for r in range(slots):
                row = jnp.broadcast_to(table[c * slots + r : c * slots + r + 1, :], (8, LANES))
                value = jnp.where(tile == r, lane_pick(row, lanes), value)
            corner[c * 8 : (c + 1) * 8, b * LANES : (b + 1) * LANES] = value

    strain = jnp.dot(
        stiff_ref[...], corner[...],
        precision=lax.Precision.HIGHEST, preferred_element_type=jnp.float32,
    )
    factor = modulus_ref[...] * weight_ref[...]
    rest = factor * (strain + strain * strain * strain * (1.0 / 3.0))
    for s in range(SPLITS):
        piece = rest.astype(jnp.bfloat16).astype(jnp.float32)
        pieces[s * 24 : (s + 1) * 24, :] = piece
        rest = rest - piece

    for b in range(blocks):
        part = slice(b * LANES, (b + 1) * LANES)
        for a in range(8):
            at = slice(a * elements + b * LANES, a * elements + (b + 1) * LANES)
            hot = high_ref[:, at]
            for g in range(SPLITS * 3):
                row = pieces[g * 8 + a : g * 8 + a + 1, part]
                value = jnp.broadcast_to(row, (16, LANES)).astype(jnp.bfloat16)
                spread[g * 16 : (g + 1) * 16, at] = hot * value
    nodal = lax.dot_general(
        spread[...], low_ref[...], (((1,), (1,)), ((), ())), preferred_element_type=jnp.float32
    )
    total = nodal[0:48]
    for s in range(1, SPLITS):
        total = total + nodal[s * 48 : (s + 1) * 48]

    places = []
    for c in range(3):
        for r in range(slots):
            row = jnp.broadcast_to(total[c * 16 + r : c * 16 + r + 1], (8, LANES))
            if r < tiles:
                places.append((dense_ref, (c * tiles + r) * modes, row))
            else:
                places.append((sides[r - tiles], c * modes, jnp.where(present[r - tiles], row, 0.0)))

    def body(k, carry):
        sums = [jnp.zeros((8, LANES), jnp.float32) for _ in range(3)]
        for i, (ref, at, row) in enumerate(places):
            sums[i % 3] = sums[i % 3] + ref[eight(at + k * 8), :] * row
        cols[eight(k * 8), :] = sums[0] + sums[1] + sums[2]
        return carry

    lax.fori_loop(0, modes // 8, body, 0, unroll=2)
    sums = jnp.sum(jnp.transpose(cols[...]), axis=0, keepdims=True)
    sums = jnp.concatenate([sums, jnp.zeros((1, 4 * LANES - modes), jnp.float32)], axis=1)
    pair = [sums[:, r * LANES : (r + 1) * LANES] for r in range(4)]
    pair = jnp.concatenate(pair + pair, axis=0)
    out_ref[...] = jnp.broadcast_to(pair[None], (out_ref.shape[0] // 8, 8, LANES)).reshape(out_ref.shape)


def step(first, parts, dense, sides, links, low, high, modulus, weight, stiffness, vectors, devices):
    modes = vectors[0].shape[1]
    tiles = dense.shape[0] // (3 * modes)
    elements = links.shape[1]
    slots = tiles + 4
    vector = jax.ShapeDtypeStruct((1, modes), jnp.float32)
    outs = [jax.ShapeDtypeStruct((devices * 4, LANES), jnp.float32)]
    args = [parts, dense, *sides, links, low, high, modulus, weight, stiffness]
    if first:
        args += vectors[:1]
    else:
        args += vectors
        outs += [vector, vector]
    return pl.pallas_call(
        functools.partial(step_kernel, first, modes, tiles),
        out_shape=tuple(outs),
        in_specs=[VMEM] * len(args),
        out_specs=(VMEM,) * len(outs),
        scratch_shapes=[
            pltpu.VMEM((modes, LANES), jnp.float32),
            pltpu.VMEM((-(-3 * slots // 8) * 8, LANES), jnp.float32),
            pltpu.VMEM((24, elements), jnp.float32),
            pltpu.VMEM((SPLITS * 24, elements), jnp.float32),
            pltpu.VMEM((SPLITS * 48, 8 * elements), jnp.bfloat16),
        ],
        compiler_params=pltpu.CompilerParams(vmem_limit_bytes=24 * MIB),
        name="first_step" if first else "next_step",
    )(*args)


def final_kernel(modes, tiles, parts_ref, dense_ref, coords_ref, velocity_ref, external_ref,
                 coords_out, velocity_out, reduced_out, displaced_out, cols):
    coords, velocity, reduced = advance(parts_ref, coords_ref, velocity_ref, external_ref)
    coords_out[...] = coords
    velocity_out[...] = velocity
    reduced_out[...] = reduced
    cols[...] = column(coords)
    for i, row in enumerate(contract(owned_places(dense_ref, modes, tiles), cols, modes)):
        c, t = divmod(i, tiles)
        displaced_out[c, :, t * LANES : (t + 1) * LANES] = row


def finish(parts, dense, vectors):
    modes = vectors[0].shape[1]
    tiles = dense.shape[0] // (3 * modes)
    vector = jax.ShapeDtypeStruct((1, modes), jnp.float32)
    return pl.pallas_call(
        functools.partial(final_kernel, modes, tiles),
        out_shape=(vector, vector, vector, jax.ShapeDtypeStruct((3, 1, tiles * LANES), jnp.float32)),
        in_specs=[VMEM] * 5,
        out_specs=(VMEM,) * 4,
        scratch_shapes=[pltpu.VMEM((modes, LANES), jnp.float32)],
        compiler_params=pltpu.CompilerParams(vmem_limit_bytes=16 * MIB),
        name="finish",
    )(parts, dense, *vectors)


def exchange(below, above, axis):
    count = lax.axis_size(axis)
    up = [(i, (i + 1) % count) for i in range(count)]
    down = [(j, i) for i, j in up]
    return lax.ppermute(above, axis, up), lax.ppermute(below, axis, down)


def everyone(parts, devices):
    chunks = parts.reshape(devices, parts.shape[0] // devices, LANES)
    return lax.all_to_all(chunks, ("gx", "gy"), 0, 0, tiled=True).reshape(parts.shape)


def shards(basis, connectivity, send_nodes, modulus, ecsw_weight, stiffness, coords, velocity, external):
    modes = coords.shape[0]
    nodes = basis.shape[3]
    flat = basis.reshape(3 * modes * nodes // LANES, LANES)
    links = connectivity[:, 0, :]
    coords, velocity, external = (x[None, :] for x in (coords, velocity, external))
    devices = lax.axis_size("gx") * lax.axis_size("gy")

    dense, below_x, above_x, below_y, above_y = load(flat, send_nodes, modes)
    r0, r1 = exchange(below_x, above_x, "gx")
    r2, r3 = exchange(below_y, above_y, "gy")
    owned, low, high = prepare(dense, links, coords)
    sides = (r0, r1, r2, r3)

    (parts,) = step(True, owned, dense, sides, links, low, high, modulus, ecsw_weight, stiffness, (coords,), devices)
    for _ in range(STEPS - 1):
        parts, coords, velocity = step(
            False, everyone(parts, devices), dense, sides, links, low, high, modulus, ecsw_weight, stiffness,
            (coords, velocity, external), devices,
        )
    coords, velocity, reduced, displaced = finish(everyone(parts, devices), dense, (coords, velocity, external))
    return coords[0], velocity[0], reduced[0], displaced


def solution(mesh):
    return jax.shard_map(
        shards,
        mesh=mesh,
        in_specs=(
            P(None, None, "gx", "gy"),
            P(None, "gx", "gy"),
            P(None, "gx", "gy"),
            P("gx", "gy"),
            P("gx", "gy"),
            P(),
            P(),
            P(),
            P(),
        ),
        out_specs=(P(), P(), P(), P(None, "gx", "gy")),
        check_vma=False,
    )
```

```python
import functools

import jax
import jax.numpy as jnp
from jax import lax
from jax.experimental import pallas as pl
from jax.experimental.pallas import tpu as pltpu
from jax.sharding import PartitionSpec as P

STEPS = 2
DT = 0.05
LANES = 128
SPLITS = 3
PIECES = 2
BOUNDS = (0, 400)
MIB = 2**20

VMEM = pl.BlockSpec(memory_space=pltpu.VMEM)
HBM = pl.BlockSpec(memory_space=pltpu.HBM)


def lane_pick(rows, lanes):
    return jnp.take_along_axis(rows, lanes, axis=1, mode="promise_in_bounds")


def eight(start):
    return pl.ds(pl.multiple_of(start, 8), 8)


def load_kernel(modes, tiles, bounds, basis_ref, send_hbm, buf, *refs):
    outs, (send_ref, hot_ref, piece_ref, sems, send_sem) = refs[:4], refs[4:]
    chunks = [(c, lo, hi) for c in range(3) for lo, hi in zip(bounds, bounds[1:])]
    copies = []
    for i, (c, lo, hi) in enumerate(chunks):
        part = pl.ds((c * modes + lo) * tiles, (hi - lo) * tiles)
        copies.append(pltpu.make_async_copy(basis_ref.at[part], buf.at[part], sems.at[i]))
    lists = pltpu.make_async_copy(send_hbm, send_ref, send_sem)
    lists.start()
    for copy in copies:
        copy.start()
    lists.wait()
    for t in range(tiles):
        count = lax.broadcasted_iota(jnp.int32, (LANES, LANES), 0) + t * LANES
        for side in range(2):
            hot = jnp.broadcast_to(send_ref[2 + side], (LANES, LANES)) == count
            hot_ref[t * LANES : (t + 1) * LANES, side * LANES : (side + 1) * LANES] = jnp.where(
                hot, 1.0, 0.0
            ).astype(jnp.bfloat16)
    picks = []
    for side in range(2):
        nodes = jnp.broadcast_to(send_ref[side], (8, LANES))
        picks.append((nodes & (LANES - 1), nodes >> 7))

    def split(i):
        c, lo, hi = chunks[i]
        copies[i].wait()
        for m in range(lo, hi, 16):
            for t in range(tiles):
                at = (c * modes + m) * tiles + t
                rows = [buf[pl.ds(at + 8 * tiles * h, 8, stride=tiles), :] for h in range(2)]
                rest = jnp.concatenate(rows, axis=0)
                for s in range(PIECES):
                    piece = rest.astype(jnp.bfloat16)
                    piece_ref[s, c * modes + m : c * modes + m + 16, t * LANES : (t + 1) * LANES] = piece
                    if s + 1 < PIECES:
                        rest = rest - piece.astype(jnp.float32)

    def pick(i):
        c, lo, hi = chunks[i]
        at = slice(c * modes + lo, c * modes + hi)
        total = None
        for s in range(PIECES):
            part = jnp.dot(piece_ref[s, at, :], hot_ref[...], preferred_element_type=jnp.float32)
            total = part if total is None else total + part
        outs[2][at, :] = total[:, :LANES]
        outs[3][at, :] = total[:, LANES:]

    def permute(i):
        c, lo, hi = chunks[i]
        for m in range(c * modes + lo, c * modes + hi, 8):
            sums = [jnp.zeros((8, LANES), jnp.float32) for _ in range(2)]
            for t in range(tiles):
                rows = buf[pl.ds(m * tiles + t, 8, stride=tiles), :]
                for side, (lanes, tile) in enumerate(picks):
                    sums[side] = jnp.where(tile == t, lane_pick(rows, lanes), sums[side])
            for side in range(2):
                outs[side][m : m + 8, :] = sums[side]

    split(0)
    for i in range(len(chunks)):
        permute(i)
        pick(i)
        if i + 1 < len(chunks):
            split(i + 1)


def load(basis, send, modes):
    rows = basis.shape[0]
    tiles = rows // (3 * modes)
    bounds = BOUNDS
    shared = jax.ShapeDtypeStruct((3 * modes, LANES), jnp.float32)
    basis = pltpu.with_memory_space_constraint(basis, pltpu.HBM)
    send = pltpu.with_memory_space_constraint(send, pltpu.HBM)
    return pl.pallas_call(
        functools.partial(load_kernel, modes, tiles, bounds),
        out_shape=(jax.ShapeDtypeStruct(basis.shape, jnp.float32),) + (shared,) * 4,
        in_specs=[HBM, HBM],
        out_specs=(VMEM,) * 5,
        scratch_shapes=[
            pltpu.VMEM(send.shape, jnp.int32),
            pltpu.VMEM((tiles * LANES, 2 * LANES), jnp.bfloat16),
            pltpu.VMEM((PIECES, 3 * modes, tiles * LANES), jnp.bfloat16),
            pltpu.SemaphoreType.DMA((3 * (len(bounds) - 1),)),
            pltpu.SemaphoreType.DMA,
        ],
        compiler_params=pltpu.CompilerParams(vmem_limit_bytes=32 * MIB),
        name="load",
    )(basis, send)


def edges():
    x, y = lax.axis_index("gx"), lax.axis_index("gy")
    return x > 0, x < lax.axis_size("gx") - 1, y > 0, y < lax.axis_size("gy") - 1


def column(row):
    return jnp.transpose(jnp.broadcast_to(row, (LANES, row.shape[1])))


def rows_of(place, k):
    ref, at, stride = place
    if stride == 1:
        return ref[eight(at + k * 8), :]
    return ref[pl.ds(at + k * (8 * stride), 8, stride=stride), :]


def contract(places, cols, modes):
    def body(k, sums):
        scale = cols[eight(k * 8), :]
        return tuple(s + rows_of(place, k) * scale for s, place in zip(sums, places))

    zero = jnp.zeros((8, LANES), jnp.float32)
    sums = lax.fori_loop(0, modes // 8, body, (zero,) * len(places), unroll=2)
    return [jnp.sum(s, axis=0, keepdims=True) for s in sums]


def owned_places(dense_ref, modes, tiles):
    return [(dense_ref, c * modes * tiles + t, tiles) for c in range(3) for t in range(tiles)]


def shared_places(sides, modes):
    return [(side, c * modes, 1) for c in range(3) for side in sides]


def prepare_kernel(modes, tiles, dense_ref, links_ref, coords_ref, owned_ref, low_ref, high_ref, cols):
    cols[...] = column(coords_ref[...])
    for i, row in enumerate(contract(owned_places(dense_ref, modes, tiles), cols, modes)):
        owned_ref[i : i + 1, :] = row
    elements = links_ref.shape[1]
    for b in range(elements // LANES):
        for a in range(8):
            links = links_ref[a : a + 1, b * LANES : (b + 1) * LANES]
            at = slice(a * elements + b * LANES, a * elements + (b + 1) * LANES)
            for ref, bits, size in ((low_ref, links & (LANES - 1), LANES), (high_ref, links >> 7, 16)):
                count = lax.broadcasted_iota(jnp.int32, (size, LANES), 0)
                hot = jnp.broadcast_to(bits, (size, LANES)) == count
                ref[:, at] = jnp.where(hot, 1.0, 0.0).astype(jnp.bfloat16)


def prepare(dense, links, coords):
    modes = coords.shape[1]
    tiles = dense.shape[0] // (3 * modes)
    entries = 8 * links.shape[1]
    return pl.pallas_call(
        functools.partial(prepare_kernel, modes, tiles),
        out_shape=(
            jax.ShapeDtypeStruct((-(-3 * tiles // 8) * 8, LANES), jnp.float32),
            jax.ShapeDtypeStruct((LANES, entries), jnp.bfloat16),
            jax.ShapeDtypeStruct((16, entries), jnp.bfloat16),
        ),
        in_specs=[VMEM] * 3,
        out_specs=(VMEM,) * 3,
        scratch_shapes=[pltpu.VMEM((modes, LANES), jnp.float32)],
        compiler_params=pltpu.CompilerParams(vmem_limit_bytes=16 * MIB),
        name="prepare",
    )(dense, links, coords)


def advance(parts_ref, coords_ref, velocity_ref, external_ref):
    sums = jnp.sum(parts_ref[...].reshape(-1, 8, LANES), axis=0)
    pair = sums[0:4] + sums[4:8]
    modes = coords_ref.shape[1]
    reduced = jnp.concatenate([pair[r : r + 1] for r in range(4)], axis=1)[:, :modes]
    velocity = velocity_ref[...] + DT * (external_ref[...] - reduced)
    coords = coords_ref[...] + DT * velocity
    return coords, velocity, reduced


def step_kernel(first, modes, tiles, *refs):
    if first:
        (owned_ref, dense_ref, r0, r1, r2, r3, links_ref, low_ref, high_ref, modulus_ref, weight_ref, stiff_ref,
         coords_ref, out_ref, cols, table, corner, pieces, spread) = refs
        coords = coords_ref[...]
    else:
        (parts_ref, dense_ref, r0, r1, r2, r3, links_ref, low_ref, high_ref, modulus_ref, weight_ref, stiff_ref,
         coords_ref, velocity_ref, external_ref, out_ref, coords_out, velocity_out,
         cols, table, corner, pieces, spread) = refs
        coords, velocity, _ = advance(parts_ref, coords_ref, velocity_ref, external_ref)
        coords_out[...] = coords
        velocity_out[...] = velocity
    sides = (r0, r1, r2, r3)
    present = edges()
    slots = tiles + 4
    elements = links_ref.shape[1]
    blocks = elements // LANES

    cols[...] = column(coords)
    if first:
        owned = [owned_ref[i : i + 1, :] for i in range(3 * tiles)]
        shared = contract(shared_places(sides, modes), cols, modes)
    else:
        rows = contract(
            owned_places(dense_ref, modes, tiles) + shared_places(sides, modes), cols, modes
        )
        owned, shared = rows[: 3 * tiles], rows[3 * tiles :]
    for c in range(3):
        rows = owned[c * tiles : (c + 1) * tiles]
        rows += [jnp.where(here, row, 0.0) for here, row in zip(present, shared[c * 4 : (c + 1) * 4])]
        for r, row in enumerate(rows):
            table[c * slots + r : c * slots + r + 1, :] = row

    for b in range(blocks):
        links = links_ref[:, b * LANES : (b + 1) * LANES]
        lanes, tile = links & (LANES - 1), links >> 7
        for c in range(3):
            value = jnp.zeros((8, LANES), jnp.float32)
            for r in range(slots):
                row = jnp.broadcast_to(table[c * slots + r : c * slots + r + 1, :], (8, LANES))
                value = jnp.where(tile == r, lane_pick(row, lanes), value)
            corner[c * 8 : (c + 1) * 8, b * LANES : (b + 1) * LANES] = value

    strain = jnp.dot(
        stiff_ref[...], corner[...],
        precision=lax.Precision.HIGHEST, preferred_element_type=jnp.float32,
    )
    factor = modulus_ref[...] * weight_ref[...]
    rest = factor * (strain + strain * strain * strain * (1.0 / 3.0))
    for s in range(SPLITS):
        piece = rest.astype(jnp.bfloat16).astype(jnp.float32)
        pieces[s * 24 : (s + 1) * 24, :] = piece
        rest = rest - piece

    for b in range(blocks):
        part = slice(b * LANES, (b + 1) * LANES)
        for a in range(8):
            at = slice(a * elements + b * LANES, a * elements + (b + 1) * LANES)
            hot = high_ref[:, at]
            for g in range(SPLITS * 3):
                row = pieces[g * 8 + a : g * 8 + a + 1, part]
                value = jnp.broadcast_to(row, (16, LANES)).astype(jnp.bfloat16)
                spread[g * 16 : (g + 1) * 16, at] = hot * value
    nodal = lax.dot_general(
        spread[...], low_ref[...], (((1,), (1,)), ((), ())), preferred_element_type=jnp.float32
    )
    total = nodal[0:48]
    for s in range(1, SPLITS):
        total = total + nodal[s * 48 : (s + 1) * 48]

    places = []
    for c in range(3):
        for r in range(slots):
            row = jnp.broadcast_to(total[c * 16 + r : c * 16 + r + 1], (8, LANES))
            if r < tiles:
                places.append(((dense_ref, c * modes * tiles + r, tiles), row))
            else:
                places.append(((sides[r - tiles], c * modes, 1), jnp.where(present[r - tiles], row, 0.0)))

    def body(k, carry):
        sums = [jnp.zeros((8, LANES), jnp.float32) for _ in range(3)]
        for i, (place, row) in enumerate(places):
            sums[i % 3] = sums[i % 3] + rows_of(place, k) * row
        cols[eight(k * 8), :] = sums[0] + sums[1] + sums[2]
        return carry

    lax.fori_loop(0, modes // 8, body, 0, unroll=2)
    sums = jnp.sum(jnp.transpose(cols[...]), axis=0, keepdims=True)
    sums = jnp.concatenate([sums, jnp.zeros((1, 4 * LANES - modes), jnp.float32)], axis=1)
    pair = [sums[:, r * LANES : (r + 1) * LANES] for r in range(4)]
    pair = jnp.concatenate(pair + pair, axis=0)
    out_ref[...] = jnp.broadcast_to(pair[None], (out_ref.shape[0] // 8, 8, LANES)).reshape(out_ref.shape)


def step(first, parts, dense, sides, links, low, high, modulus, weight, stiffness, vectors, devices):
    modes = vectors[0].shape[1]
    tiles = dense.shape[0] // (3 * modes)
    elements = links.shape[1]
    slots = tiles + 4
    vector = jax.ShapeDtypeStruct((1, modes), jnp.float32)
    outs = [jax.ShapeDtypeStruct((devices * 4, LANES), jnp.float32)]
    args = [parts, dense, *sides, links, low, high, modulus, weight, stiffness]
    if first:
        args += vectors[:1]
    else:
        args += vectors
        outs += [vector, vector]
    return pl.pallas_call(
        functools.partial(step_kernel, first, modes, tiles),
        out_shape=tuple(outs),
        in_specs=[VMEM] * len(args),
        out_specs=(VMEM,) * len(outs),
        scratch_shapes=[
            pltpu.VMEM((modes, LANES), jnp.float32),
            pltpu.VMEM((-(-3 * slots // 8) * 8, LANES), jnp.float32),
            pltpu.VMEM((24, elements), jnp.float32),
            pltpu.VMEM((SPLITS * 24, elements), jnp.float32),
            pltpu.VMEM((SPLITS * 48, 8 * elements), jnp.bfloat16),
        ],
        compiler_params=pltpu.CompilerParams(vmem_limit_bytes=24 * MIB),
        name="first_step" if first else "next_step",
    )(*args)


def final_kernel(modes, tiles, parts_ref, dense_ref, coords_ref, velocity_ref, external_ref,
                 coords_out, velocity_out, reduced_out, displaced_out, cols):
    coords, velocity, reduced = advance(parts_ref, coords_ref, velocity_ref, external_ref)
    coords_out[...] = coords
    velocity_out[...] = velocity
    reduced_out[...] = reduced
    cols[...] = column(coords)
    for i, row in enumerate(contract(owned_places(dense_ref, modes, tiles), cols, modes)):
        c, t = divmod(i, tiles)
        displaced_out[c, :, t * LANES : (t + 1) * LANES] = row


def finish(parts, dense, vectors):
    modes = vectors[0].shape[1]
    tiles = dense.shape[0] // (3 * modes)
    vector = jax.ShapeDtypeStruct((1, modes), jnp.float32)
    return pl.pallas_call(
        functools.partial(final_kernel, modes, tiles),
        out_shape=(vector, vector, vector, jax.ShapeDtypeStruct((3, 1, tiles * LANES), jnp.float32)),
        in_specs=[VMEM] * 5,
        out_specs=(VMEM,) * 4,
        scratch_shapes=[pltpu.VMEM((modes, LANES), jnp.float32)],
        compiler_params=pltpu.CompilerParams(vmem_limit_bytes=16 * MIB),
        name="finish",
    )(parts, dense, *vectors)


def exchange(below, above, axis):
    count = lax.axis_size(axis)
    up = [(i, (i + 1) % count) for i in range(count)]
    down = [(j, i) for i, j in up]
    return lax.ppermute(above, axis, up), lax.ppermute(below, axis, down)


def everyone(parts, devices):
    chunks = parts.reshape(devices, parts.shape[0] // devices, LANES)
    return lax.all_to_all(chunks, ("gx", "gy"), 0, 0, tiled=True).reshape(parts.shape)


def shards(basis, connectivity, send_nodes, modulus, ecsw_weight, stiffness, coords, velocity, external):
    modes = coords.shape[0]
    nodes = basis.shape[3]
    flat = basis.reshape(3 * modes * nodes // LANES, LANES)
    links = connectivity[:, 0, :]
    coords, velocity, external = (x[None, :] for x in (coords, velocity, external))
    devices = lax.axis_size("gx") * lax.axis_size("gy")

    dense, below_x, above_x, below_y, above_y = load(flat, send_nodes, modes)
    r0, r1 = exchange(below_x, above_x, "gx")
    r2, r3 = exchange(below_y, above_y, "gy")
    owned, low, high = prepare(dense, links, coords)
    sides = (r0, r1, r2, r3)

    (parts,) = step(True, owned, dense, sides, links, low, high, modulus, ecsw_weight, stiffness, (coords,), devices)
    for _ in range(STEPS - 1):
        parts, coords, velocity = step(
            False, everyone(parts, devices), dense, sides, links, low, high, modulus, ecsw_weight, stiffness,
            (coords, velocity, external), devices,
        )
    coords, velocity, reduced, displaced = finish(everyone(parts, devices), dense, (coords, velocity, external))
    return coords[0], velocity[0], reduced[0], displaced


def solution(mesh):
    return jax.shard_map(
        shards,
        mesh=mesh,
        in_specs=(
            P(None, None, "gx", "gy"),
            P(None, "gx", "gy"),
            P(None, "gx", "gy"),
            P("gx", "gy"),
            P("gx", "gy"),
            P(),
            P(),
            P(),
            P(),
        ),
        out_specs=(P(), P(), P(), P(None, "gx", "gy")),
        check_vma=False,
    )
```

```python
import functools

import jax
import jax.numpy as jnp
from jax import lax
from jax.experimental import pallas as pl
from jax.experimental.pallas import tpu as pltpu
from jax.sharding import PartitionSpec as P


STEPS = 2
DT = 0.05
LANES = 128
SPLITS = 2
PIECES = 2
MIB = 2**20

VMEM = pl.BlockSpec(memory_space=pltpu.VMEM)
HBM = pl.BlockSpec(memory_space=pltpu.HBM)


def lane_pick(rows, lanes):
    return jnp.take_along_axis(rows, lanes, axis=1, mode="promise_in_bounds")


def eight(start):
    return pl.ds(pl.multiple_of(start, 8), 8)


def load_kernel(modes, tiles, basis_ref, send_hbm, buf, piece_ref, hot_ref, below_ref, above_ref,
                send_ref, hot_y, sems, send_sem):
    size = modes * tiles
    copies = []
    for c in range(3):
        part = pl.ds(c * size, size)
        copies.append(pltpu.make_async_copy(basis_ref.at[part], buf.at[part], sems.at[c]))
    lists = pltpu.make_async_copy(send_hbm, send_ref, send_sem)
    lists.start()
    for copy in copies:
        copy.start()
    lists.wait()
    for t in range(tiles):
        count = lax.broadcasted_iota(jnp.int32, (LANES, LANES), 0) + t * LANES
        for side in range(4):
            ref = hot_ref if side < 2 else hot_y
            hot = jnp.broadcast_to(send_ref[side], (LANES, LANES)) == count
            at = (side % 2) * LANES
            ref[t * LANES : (t + 1) * LANES, at : at + LANES] = jnp.where(hot, 1.0, 0.0).astype(jnp.bfloat16)

    def split(c):
        copies[c].wait()
        for m in range(c * modes, (c + 1) * modes, 16):
            for t in range(tiles):
                rows = [buf[pl.ds((m + 8 * h) * tiles + t, 8, stride=tiles), :] for h in range(2)]
                rest = jnp.concatenate(rows, axis=0)
                for s in range(PIECES):
                    piece = rest.astype(jnp.bfloat16)
                    piece_ref[s, m : m + 16, t * LANES : (t + 1) * LANES] = piece
                    if s + 1 < PIECES:
                        rest = rest - piece.astype(jnp.float32)

    split(0)
    for c in range(3):
        if c < 2:
            split(c + 1)
        pick(c, modes, piece_ref, hot_y, below_ref, above_ref)


def pick(c, modes, piece_ref, hot_ref, below_ref, above_ref):
    at = slice(c * modes, (c + 1) * modes)
    total = None
    for s in range(PIECES):
        part = jnp.dot(piece_ref[s, at, :], hot_ref[...], preferred_element_type=jnp.float32)
        total = part if total is None else total + part
    below_ref[at, :] = total[:, :LANES]
    above_ref[at, :] = total[:, LANES:]


def load(basis, send, modes):
    rows = basis.shape[0]
    tiles = rows // (3 * modes)
    shared = jax.ShapeDtypeStruct((3 * modes, LANES), jnp.float32)
    hot = (tiles * LANES, 2 * LANES)
    basis = pltpu.with_memory_space_constraint(basis, pltpu.HBM)
    send = pltpu.with_memory_space_constraint(send, pltpu.HBM)
    return pl.pallas_call(
        functools.partial(load_kernel, modes, tiles),
        out_shape=(
            jax.ShapeDtypeStruct(basis.shape, jnp.float32),
            jax.ShapeDtypeStruct((PIECES, 3 * modes, tiles * LANES), jnp.bfloat16),
            jax.ShapeDtypeStruct(hot, jnp.bfloat16),
            shared,
            shared,
        ),
        in_specs=[HBM, HBM],
        out_specs=(VMEM,) * 5,
        scratch_shapes=[
            pltpu.VMEM(send.shape, jnp.int32),
            pltpu.VMEM(hot, jnp.bfloat16),
            pltpu.SemaphoreType.DMA((3,)),
            pltpu.SemaphoreType.DMA,
        ],
        compiler_params=pltpu.CompilerParams(vmem_limit_bytes=24 * MIB),
        name="load",
    )(basis, send)


def share_kernel(modes, piece_ref, hot_ref, below_ref, above_ref):
    for c in range(3):
        pick(c, modes, piece_ref, hot_ref, below_ref, above_ref)


def share(pieces, hot, modes):
    shared = jax.ShapeDtypeStruct((3 * modes, LANES), jnp.float32)
    return pl.pallas_call(
        functools.partial(share_kernel, modes),
        out_shape=(shared, shared),
        in_specs=[VMEM, VMEM],
        out_specs=(VMEM,) * 2,
        compiler_params=pltpu.CompilerParams(vmem_limit_bytes=16 * MIB),
        name="share",
    )(pieces, hot)


def edges():
    x, y = lax.axis_index("gx"), lax.axis_index("gy")
    return x > 0, x < lax.axis_size("gx") - 1, y > 0, y < lax.axis_size("gy") - 1


def column(row):
    return jnp.transpose(jnp.broadcast_to(row, (LANES, row.shape[1])))


def rows_of(place, k):
    ref, at, stride = place
    if stride == 1:
        return ref[eight(at + k * 8), :]
    return ref[pl.ds(at + k * (8 * stride), 8, stride=stride), :]


def contract(places, cols, modes):
    def body(k, sums):
        scale = cols[eight(k * 8), :]
        return tuple(s + rows_of(place, k) * scale for s, place in zip(sums, places))

    zero = jnp.zeros((8, LANES), jnp.float32)
    sums = lax.fori_loop(0, modes // 8, body, (zero,) * len(places), unroll=2)
    return [jnp.sum(s, axis=0, keepdims=True) for s in sums]


def owned_places(dense_ref, modes, tiles):
    return [(dense_ref, c * modes * tiles + t, tiles) for c in range(3) for t in range(tiles)]


def shared_places(sides, modes):
    return [(side, c * modes, 1) for c in range(3) for side in sides]


def prepare_kernel(modes, tiles, dense_ref, links_ref, coords_ref, owned_ref, low_ref, high_ref, cols):
    cols[...] = column(coords_ref[...])
    for i, row in enumerate(contract(owned_places(dense_ref, modes, tiles), cols, modes)):
        owned_ref[i : i + 1, :] = row
    elements = links_ref.shape[1]
    for b in range(elements // LANES):
        for a in range(8):
            links = links_ref[a : a + 1, b * LANES : (b + 1) * LANES]
            at = slice(a * elements + b * LANES, a * elements + (b + 1) * LANES)
            for ref, bits, size in ((low_ref, links & (LANES - 1), LANES), (high_ref, links >> 7, 16)):
                count = lax.broadcasted_iota(jnp.int32, (size, LANES), 0)
                hot = jnp.broadcast_to(bits, (size, LANES)) == count
                ref[:, at] = jnp.where(hot, 1.0, 0.0).astype(jnp.bfloat16)


def prepare(dense, links, coords):
    modes = coords.shape[1]
    tiles = dense.shape[0] // (3 * modes)
    entries = 8 * links.shape[1]
    return pl.pallas_call(
        functools.partial(prepare_kernel, modes, tiles),
        out_shape=(
            jax.ShapeDtypeStruct((-(-3 * tiles // 8) * 8, LANES), jnp.float32),
            jax.ShapeDtypeStruct((LANES, entries), jnp.bfloat16),
            jax.ShapeDtypeStruct((16, entries), jnp.bfloat16),
        ),
        in_specs=[VMEM] * 3,
        out_specs=(VMEM,) * 3,
        scratch_shapes=[pltpu.VMEM((modes, LANES), jnp.float32)],
        compiler_params=pltpu.CompilerParams(vmem_limit_bytes=16 * MIB),
        name="prepare",
    )(dense, links, coords)


def advance(parts_ref, coords_ref, velocity_ref, external_ref):
    sums = jnp.sum(parts_ref[...].reshape(-1, 8, LANES), axis=0)
    pair = sums[0:4] + sums[4:8]
    modes = coords_ref.shape[1]
    reduced = jnp.concatenate([pair[r : r + 1] for r in range(4)], axis=1)[:, :modes]
    velocity = velocity_ref[...] + DT * (external_ref[...] - reduced)
    coords = coords_ref[...] + DT * velocity
    return coords, velocity, reduced


def step_kernel(first, modes, tiles, *refs):
    if first:
        (owned_ref, dense_ref, r0, r1, r2, r3, links_ref, low_ref, high_ref, modulus_ref, weight_ref, stiff_ref,
         coords_ref, out_ref, cols, table, corner, pieces, spread) = refs
        coords = coords_ref[...]
    else:
        (parts_ref, dense_ref, r0, r1, r2, r3, links_ref, low_ref, high_ref, modulus_ref, weight_ref, stiff_ref,
         coords_ref, velocity_ref, external_ref, out_ref, coords_out, velocity_out,
         cols, table, corner, pieces, spread) = refs
        coords, velocity, _ = advance(parts_ref, coords_ref, velocity_ref, external_ref)
        coords_out[...] = coords
        velocity_out[...] = velocity
    sides = (r0, r1, r2, r3)
    present = edges()
    slots = tiles + 4
    elements = links_ref.shape[1]
    blocks = elements // LANES

    cols[...] = column(coords)
    if first:
        owned = [owned_ref[i : i + 1, :] for i in range(3 * tiles)]
        shared = contract(shared_places(sides, modes), cols, modes)
    else:
        rows = contract(
            owned_places(dense_ref, modes, tiles) + shared_places(sides, modes), cols, modes
        )
        owned, shared = rows[: 3 * tiles], rows[3 * tiles :]
    for c in range(3):
        rows = owned[c * tiles : (c + 1) * tiles]
        rows += [jnp.where(here, row, 0.0) for here, row in zip(present, shared[c * 4 : (c + 1) * 4])]
        for r, row in enumerate(rows):
            table[c * slots + r : c * slots + r + 1, :] = row

    for b in range(blocks):
        links = links_ref[:, b * LANES : (b + 1) * LANES]
        lanes, tile = links & (LANES - 1), links >> 7
        for c in range(3):
            value = jnp.zeros((8, LANES), jnp.float32)
            for r in range(slots):
                row = jnp.broadcast_to(table[c * slots + r : c * slots + r + 1, :], (8, LANES))
                value = jnp.where(tile == r, lane_pick(row, lanes), value)
            corner[c * 8 : (c + 1) * 8, b * LANES : (b + 1) * LANES] = value

    strain = jnp.dot(
        stiff_ref[...], corner[...],
        precision=lax.Precision.HIGHEST, preferred_element_type=jnp.float32,
    )
    factor = modulus_ref[...] * weight_ref[...]
    rest = factor * (strain + strain * strain * strain * (1.0 / 3.0))
    for s in range(SPLITS):
        piece = rest.astype(jnp.bfloat16).astype(jnp.float32)
        pieces[s * 24 : (s + 1) * 24, :] = piece
        rest = rest - piece

    for b in range(blocks):
        part = slice(b * LANES, (b + 1) * LANES)
        for a in range(8):
            at = slice(a * elements + b * LANES, a * elements + (b + 1) * LANES)
            hot = high_ref[:, at]
            for g in range(SPLITS * 3):
                row = pieces[g * 8 + a : g * 8 + a + 1, part]
                value = jnp.broadcast_to(row, (16, LANES)).astype(jnp.bfloat16)
                spread[g * 16 : (g + 1) * 16, at] = hot * value
    nodal = lax.dot_general(
        spread[...], low_ref[...], (((1,), (1,)), ((), ())), preferred_element_type=jnp.float32
    )
    total = nodal[0:48]
    for s in range(1, SPLITS):
        total = total + nodal[s * 48 : (s + 1) * 48]

    places = []
    for c in range(3):
        for r in range(slots):
            row = jnp.broadcast_to(total[c * 16 + r : c * 16 + r + 1], (8, LANES))
            if r < tiles:
                places.append(((dense_ref, c * modes * tiles + r, tiles), row))
            else:
                places.append(((sides[r - tiles], c * modes, 1), jnp.where(present[r - tiles], row, 0.0)))

    def body(k, carry):
        sums = [jnp.zeros((8, LANES), jnp.float32) for _ in range(3)]
        for i, (place, row) in enumerate(places):
            sums[i % 3] = sums[i % 3] + rows_of(place, k) * row
        cols[eight(k * 8), :] = sums[0] + sums[1] + sums[2]
        return carry

    lax.fori_loop(0, modes // 8, body, 0, unroll=2)
    sums = jnp.sum(jnp.transpose(cols[...]), axis=0, keepdims=True)
    sums = jnp.concatenate([sums, jnp.zeros((1, 4 * LANES - modes), jnp.float32)], axis=1)
    pair = [sums[:, r * LANES : (r + 1) * LANES] for r in range(4)]
    pair = jnp.concatenate(pair + pair, axis=0)
    out_ref[...] = jnp.broadcast_to(pair[None], (out_ref.shape[0] // 8, 8, LANES)).reshape(out_ref.shape)


def step(first, parts, dense, sides, links, low, high, modulus, weight, stiffness, vectors, devices):
    modes = vectors[0].shape[1]
    tiles = dense.shape[0] // (3 * modes)
    elements = links.shape[1]
    slots = tiles + 4
    vector = jax.ShapeDtypeStruct((1, modes), jnp.float32)
    outs = [jax.ShapeDtypeStruct((devices * 4, LANES), jnp.float32)]
    args = [parts, dense, *sides, links, low, high, modulus, weight, stiffness]
    if first:
        args += vectors[:1]
    else:
        args += vectors
        outs += [vector, vector]
    return pl.pallas_call(
        functools.partial(step_kernel, first, modes, tiles),
        out_shape=tuple(outs),
        in_specs=[VMEM] * len(args),
        out_specs=(VMEM,) * len(outs),
        scratch_shapes=[
            pltpu.VMEM((modes, LANES), jnp.float32),
            pltpu.VMEM((-(-3 * slots // 8) * 8, LANES), jnp.float32),
            pltpu.VMEM((24, elements), jnp.float32),
            pltpu.VMEM((SPLITS * 24, elements), jnp.float32),
            pltpu.VMEM((SPLITS * 48, 8 * elements), jnp.bfloat16),
        ],
        compiler_params=pltpu.CompilerParams(vmem_limit_bytes=24 * MIB),
        name="first_step" if first else "next_step",
    )(*args)


def final_kernel(modes, tiles, parts_ref, dense_ref, coords_ref, velocity_ref, external_ref,
                 coords_out, velocity_out, reduced_out, displaced_out, cols):
    coords, velocity, reduced = advance(parts_ref, coords_ref, velocity_ref, external_ref)
    coords_out[...] = coords
    velocity_out[...] = velocity
    reduced_out[...] = reduced
    cols[...] = column(coords)
    for i, row in enumerate(contract(owned_places(dense_ref, modes, tiles), cols, modes)):
        c, t = divmod(i, tiles)
        displaced_out[c, :, t * LANES : (t + 1) * LANES] = row


def finish(parts, dense, vectors):
    modes = vectors[0].shape[1]
    tiles = dense.shape[0] // (3 * modes)
    vector = jax.ShapeDtypeStruct((1, modes), jnp.float32)
    return pl.pallas_call(
        functools.partial(final_kernel, modes, tiles),
        out_shape=(vector, vector, vector, jax.ShapeDtypeStruct((3, 1, tiles * LANES), jnp.float32)),
        in_specs=[VMEM] * 5,
        out_specs=(VMEM,) * 4,
        scratch_shapes=[pltpu.VMEM((modes, LANES), jnp.float32)],
        compiler_params=pltpu.CompilerParams(vmem_limit_bytes=16 * MIB),
        name="finish",
    )(parts, dense, *vectors)


def exchange(below, above, axis):
    count = lax.axis_size(axis)
    up = [(i, (i + 1) % count) for i in range(count)]
    down = [(j, i) for i, j in up]
    return lax.ppermute(above, axis, up), lax.ppermute(below, axis, down)


def everyone(parts, devices):
    chunks = parts.reshape(devices, parts.shape[0] // devices, LANES)
    return lax.all_to_all(chunks, ("gx", "gy"), 0, 0, tiled=True).reshape(parts.shape)


def shards(basis, connectivity, send_nodes, modulus, ecsw_weight, stiffness, coords, velocity, external):
    modes = coords.shape[0]
    nodes = basis.shape[3]
    flat = basis.reshape(3 * modes * nodes // LANES, LANES)
    links = connectivity[:, 0, :]
    coords, velocity, external = (x[None, :] for x in (coords, velocity, external))
    devices = lax.axis_size("gx") * lax.axis_size("gy")

    dense, pieces, hot, below, above = load(flat, send_nodes, modes)
    r2, r3 = exchange(below, above, "gy")
    below, above = share(pieces, hot, modes)
    r0, r1 = exchange(below, above, "gx")
    owned, low, high = prepare(dense, links, coords)
    sides = (r0, r1, r2, r3)

    (parts,) = step(True, owned, dense, sides, links, low, high, modulus, ecsw_weight, stiffness, (coords,), devices)
    for _ in range(STEPS - 1):
        parts, coords, velocity = step(
            False, everyone(parts, devices), dense, sides, links, low, high, modulus, ecsw_weight, stiffness,
            (coords, velocity, external), devices,
        )
    coords, velocity, reduced, displaced = finish(everyone(parts, devices), dense, (coords, velocity, external))
    return coords[0], velocity[0], reduced[0], displaced


def solution(mesh):
    return jax.shard_map(
        shards,
        mesh=mesh,
        in_specs=(
            P(None, None, "gx", "gy"),
            P(None, "gx", "gy"),
            P(None, "gx", "gy"),
            P("gx", "gy"),
            P("gx", "gy"),
            P(),
            P(),
            P(),
            P(),
        ),
        out_specs=(P(), P(), P(), P(None, "gx", "gy")),
        check_vma=False,
    )
```

```python
import functools

import jax
import jax.numpy as jnp
from jax import lax
from jax.experimental import pallas as pl
from jax.experimental.pallas import tpu as pltpu
from jax.sharding import PartitionSpec as P


STEPS = 2
DT = 0.05
LANES = 128
SPLITS = 2
PIECES = 2
MIB = 2**20

VMEM = pl.BlockSpec(memory_space=pltpu.VMEM)
HBM = pl.BlockSpec(memory_space=pltpu.HBM)


def lane_pick(rows, lanes):
    return jnp.take_along_axis(rows, lanes, axis=1, mode="promise_in_bounds")


def eight(start):
    return pl.ds(pl.multiple_of(start, 8), 8)


def load_kernel(modes, tiles, basis_ref, send_hbm, buf, piece_ref, hot_ref, below_ref, above_ref,
                send_ref, hot_y, sems, send_sem):
    size = modes * tiles
    copies = []
    for c in range(3):
        part = pl.ds(c * size, size)
        copies.append(pltpu.make_async_copy(basis_ref.at[part], buf.at[part], sems.at[c]))
    lists = pltpu.make_async_copy(send_hbm, send_ref, send_sem)
    lists.start()
    for copy in copies:
        copy.start()
    lists.wait()
    for t in range(tiles):
        count = lax.broadcasted_iota(jnp.int32, (LANES, LANES), 0) + t * LANES
        for side in range(4):
            ref = hot_ref if side < 2 else hot_y
            hot = jnp.broadcast_to(send_ref[side], (LANES, LANES)) == count
            at = (side % 2) * LANES
            ref[t * LANES : (t + 1) * LANES, at : at + LANES] = jnp.where(hot, 1.0, 0.0).astype(jnp.bfloat16)

    def split(c):
        copies[c].wait()
        for m in range(c * modes, (c + 1) * modes, 16):
            for t in range(tiles):
                rows = [buf[pl.ds((m + 8 * h) * tiles + t, 8, stride=tiles), :] for h in range(2)]
                rest = jnp.concatenate(rows, axis=0)
                for s in range(PIECES):
                    piece = rest.astype(jnp.bfloat16)
                    piece_ref[s, m : m + 16, t * LANES : (t + 1) * LANES] = piece
                    if s + 1 < PIECES:
                        rest = rest - piece.astype(jnp.float32)

    split(0)
    for c in range(3):
        if c < 2:
            split(c + 1)
        pick(c, modes, piece_ref, hot_y, below_ref, above_ref)


def pick(c, modes, piece_ref, hot_ref, below_ref, above_ref):
    at = slice(c * modes, (c + 1) * modes)
    total = None
    for s in range(PIECES):
        part = jnp.dot(piece_ref[s, at, :], hot_ref[...], preferred_element_type=jnp.float32)
        total = part if total is None else total + part
    below_ref[at, :] = total[:, :LANES]
    above_ref[at, :] = total[:, LANES:]


def load(basis, send, modes):
    rows = basis.shape[0]
    tiles = rows // (3 * modes)
    shared = jax.ShapeDtypeStruct((3 * modes, LANES), jnp.float32)
    hot = (tiles * LANES, 2 * LANES)
    basis = pltpu.with_memory_space_constraint(basis, pltpu.HBM)
    send = pltpu.with_memory_space_constraint(send, pltpu.HBM)
    return pl.pallas_call(
        functools.partial(load_kernel, modes, tiles),
        out_shape=(
            jax.ShapeDtypeStruct(basis.shape, jnp.float32),
            jax.ShapeDtypeStruct((PIECES, 3 * modes, tiles * LANES), jnp.bfloat16),
            jax.ShapeDtypeStruct(hot, jnp.bfloat16),
            shared,
            shared,
        ),
        in_specs=[HBM, HBM],
        out_specs=(VMEM,) * 5,
        scratch_shapes=[
            pltpu.VMEM(send.shape, jnp.int32),
            pltpu.VMEM(hot, jnp.bfloat16),
            pltpu.SemaphoreType.DMA((3,)),
            pltpu.SemaphoreType.DMA,
        ],
        compiler_params=pltpu.CompilerParams(vmem_limit_bytes=24 * MIB),
        name="load",
    )(basis, send)


def share_kernel(modes, piece_ref, hot_ref, below_ref, above_ref):
    for c in range(3):
        pick(c, modes, piece_ref, hot_ref, below_ref, above_ref)


def share(pieces, hot, modes):
    shared = jax.ShapeDtypeStruct((3 * modes, LANES), jnp.float32)
    return pl.pallas_call(
        functools.partial(share_kernel, modes),
        out_shape=(shared, shared),
        in_specs=[VMEM, VMEM],
        out_specs=(VMEM,) * 2,
        compiler_params=pltpu.CompilerParams(vmem_limit_bytes=16 * MIB),
        name="share",
    )(pieces, hot)


def edges():
    x, y = lax.axis_index("gx"), lax.axis_index("gy")
    return x > 0, x < lax.axis_size("gx") - 1, y > 0, y < lax.axis_size("gy") - 1


def column(row):
    return jnp.transpose(jnp.broadcast_to(row, (LANES, row.shape[1])))


def rows_of(place, k):
    ref, at, stride = place
    if stride == 1:
        return ref[eight(at + k * 8), :]
    return ref[pl.ds(at + k * (8 * stride), 8, stride=stride), :]


def contract(places, cols, modes):
    def body(k, sums):
        scale = cols[eight(k * 8), :]
        return tuple(s + rows_of(place, k) * scale for s, place in zip(sums, places))

    zero = jnp.zeros((8, LANES), jnp.float32)
    sums = lax.fori_loop(0, modes // 8, body, (zero,) * len(places), unroll=50)
    return [jnp.sum(s, axis=0, keepdims=True) for s in sums]


def owned_places(dense_ref, modes, tiles):
    return [(dense_ref, c * modes * tiles + t, tiles) for c in range(3) for t in range(tiles)]


def shared_places(sides, modes):
    return [(side, c * modes, 1) for c in range(3) for side in sides]


def corner_values(links_ref, table, value_of, places):
    for b in range(links_ref.shape[1] // LANES):
        part = slice(b * LANES, (b + 1) * LANES)
        lanes, tile = links_ref[:, part] & (LANES - 1), links_ref[:, part] >> 7
        for c in range(3):
            value = value_of(c, part)
            for r, t in places:
                row = jnp.broadcast_to(table[c * 16 + r : c * 16 + r + 1, :], (8, LANES))
                value = jnp.where(tile == t, lane_pick(row, lanes), value)
            yield c, part, value


def prepare_kernel(modes, tiles, dense_ref, links_ref, coords_ref, corner_ref, low_ref, high_ref, cols, table):
    cols[...] = column(coords_ref[...])
    for i, row in enumerate(contract(owned_places(dense_ref, modes, tiles), cols, modes)):
        c, t = divmod(i, tiles)
        table[c * 16 + t : c * 16 + t + 1, :] = row
    zero = jnp.zeros((8, LANES), jnp.float32)
    own = [(t, t) for t in range(tiles)]
    for c, part, value in corner_values(links_ref, table, lambda c, part: zero, own):
        corner_ref[c * 8 : (c + 1) * 8, part] = value
    elements = links_ref.shape[1]
    for b in range(elements // LANES):
        for a in range(8):
            links = links_ref[a : a + 1, b * LANES : (b + 1) * LANES]
            at = slice(a * elements + b * LANES, a * elements + (b + 1) * LANES)
            count = lax.broadcasted_iota(jnp.int32, (LANES, LANES), 0)
            hot = jnp.broadcast_to(links & (LANES - 1), (LANES, LANES)) == count
            low_ref[at, :] = jnp.transpose(jnp.where(hot, 1.0, 0.0)).astype(jnp.bfloat16)
            hot = jnp.broadcast_to(links >> 7, (16, LANES)) == count[:16]
            high_ref[:, at] = jnp.where(hot, 1.0, 0.0).astype(jnp.bfloat16)


def prepare(dense, links, coords):
    modes = coords.shape[1]
    tiles = dense.shape[0] // (3 * modes)
    elements = links.shape[1]
    return pl.pallas_call(
        functools.partial(prepare_kernel, modes, tiles),
        out_shape=(
            jax.ShapeDtypeStruct((24, elements), jnp.float32),
            jax.ShapeDtypeStruct((8 * elements, LANES), jnp.bfloat16),
            jax.ShapeDtypeStruct((16, 8 * elements), jnp.bfloat16),
        ),
        in_specs=[VMEM] * 3,
        out_specs=(VMEM,) * 3,
        scratch_shapes=[pltpu.VMEM((modes, LANES), jnp.float32), pltpu.VMEM((48, LANES), jnp.float32)],
        compiler_params=pltpu.CompilerParams(vmem_limit_bytes=16 * MIB),
        name="prepare",
    )(dense, links, coords)


def advance(parts_ref, coords_ref, velocity_ref, external_ref):
    sums = jnp.sum(parts_ref[...].reshape(-1, 8, LANES), axis=0)
    pair = sums[0:4] + sums[4:8]
    modes = coords_ref.shape[1]
    reduced = jnp.concatenate([pair[r : r + 1] for r in range(4)], axis=1)[:, :modes]
    velocity = velocity_ref[...] + DT * (external_ref[...] - reduced)
    coords = coords_ref[...] + DT * velocity
    return coords, velocity, reduced


def step_kernel(first, modes, tiles, *refs):
    if first:
        (owned_ref, dense_ref, r0, r1, r2, r3, links_ref, low_ref, high_ref, modulus_ref, weight_ref, stiff_ref,
         coords_ref, out_ref, cols, table, corner, pieces, spread) = refs
        coords = coords_ref[...]
    else:
        (parts_ref, dense_ref, r0, r1, r2, r3, links_ref, low_ref, high_ref, modulus_ref, weight_ref, stiff_ref,
         coords_ref, velocity_ref, external_ref, out_ref, coords_out, velocity_out,
         cols, table, corner, pieces, spread) = refs
        coords, velocity, _ = advance(parts_ref, coords_ref, velocity_ref, external_ref)
        coords_out[...] = coords
        velocity_out[...] = velocity
    sides = (r0, r1, r2, r3)
    present = edges()
    slots = tiles + 4
    elements = links_ref.shape[1]
    blocks = elements // LANES

    cols[...] = column(coords)
    shared = shared_places(sides, modes)
    if first:
        rows = contract(shared, cols, modes)
        places = [(tiles + i, tiles + i) for i in range(4)]
        owned = []
    else:
        rows = contract(owned_places(dense_ref, modes, tiles) + shared, cols, modes)
        owned, rows = rows[: 3 * tiles], rows[3 * tiles :]
        places = [(r, r) for r in range(slots)]
    for i, row in enumerate(owned):
        c, t = divmod(i, tiles)
        table[c * 16 + t : c * 16 + t + 1, :] = row
    for i, row in enumerate(rows):
        c, side = divmod(i, 4)
        at = c * 16 + tiles + side
        table[at : at + 1, :] = jnp.where(present[side], row, 0.0)

    def start(c, part):
        return owned_ref[c * 8 : (c + 1) * 8, part] if first else jnp.zeros((8, LANES), jnp.float32)

    for c, part, value in corner_values(links_ref, table, start, places):
        corner[c * 8 : (c + 1) * 8, part] = value

    strain = jnp.dot(
        stiff_ref[...], corner[...],
        precision=lax.Precision.HIGHEST, preferred_element_type=jnp.float32,
    )
    factor = modulus_ref[...] * weight_ref[...]
    rest = factor * (strain + strain * strain * strain * (1.0 / 3.0))
    for s in range(SPLITS):
        piece = rest.astype(jnp.bfloat16).astype(jnp.float32)
        pieces[s * 24 : (s + 1) * 24, :] = piece
        rest = rest - piece

    for b in range(blocks):
        part = slice(b * LANES, (b + 1) * LANES)
        for a in range(8):
            at = slice(a * elements + b * LANES, a * elements + (b + 1) * LANES)
            hot = high_ref[:, at]
            for g in range(SPLITS * 3):
                row = pieces[g * 8 + a : g * 8 + a + 1, part]
                value = jnp.broadcast_to(row, (16, LANES)).astype(jnp.bfloat16)
                spread[g * 16 : (g + 1) * 16, at] = hot * value
    nodal = jnp.dot(spread[...], low_ref[...], preferred_element_type=jnp.float32)
    total = nodal[0:48]
    for s in range(1, SPLITS):
        total = total + nodal[s * 48 : (s + 1) * 48]

    places = []
    for c in range(3):
        for r in range(slots):
            row = jnp.broadcast_to(total[c * 16 + r : c * 16 + r + 1], (8, LANES))
            if r < tiles:
                places.append(((dense_ref, c * modes * tiles + r, tiles), row))
            else:
                places.append(((sides[r - tiles], c * modes, 1), jnp.where(present[r - tiles], row, 0.0)))

    def body(k, carry):
        sums = [jnp.zeros((8, LANES), jnp.float32) for _ in range(3)]
        for i, (place, row) in enumerate(places):
            sums[i % 3] = sums[i % 3] + rows_of(place, k) * row
        cols[eight(k * 8), :] = sums[0] + sums[1] + sums[2]
        return carry

    lax.fori_loop(0, modes // 8, body, 0, unroll=50)
    sums = jnp.sum(jnp.transpose(cols[...]), axis=0, keepdims=True)
    sums = jnp.concatenate([sums, jnp.zeros((1, 4 * LANES - modes), jnp.float32)], axis=1)
    pair = [sums[:, r * LANES : (r + 1) * LANES] for r in range(4)]
    pair = jnp.concatenate(pair + pair, axis=0)
    out_ref[...] = jnp.broadcast_to(pair[None], (out_ref.shape[0] // 8, 8, LANES)).reshape(out_ref.shape)


def step(first, parts, dense, sides, links, low, high, modulus, weight, stiffness, vectors, devices):
    modes = vectors[0].shape[1]
    tiles = dense.shape[0] // (3 * modes)
    elements = links.shape[1]
    vector = jax.ShapeDtypeStruct((1, modes), jnp.float32)
    outs = [jax.ShapeDtypeStruct((devices * 4, LANES), jnp.float32)]
    args = [parts, dense, *sides, links, low, high, modulus, weight, stiffness]
    if first:
        args += vectors[:1]
    else:
        args += vectors
        outs += [vector, vector]
    return pl.pallas_call(
        functools.partial(step_kernel, first, modes, tiles),
        out_shape=tuple(outs),
        in_specs=[VMEM] * len(args),
        out_specs=(VMEM,) * len(outs),
        scratch_shapes=[
            pltpu.VMEM((modes, LANES), jnp.float32),
            pltpu.VMEM((48, LANES), jnp.float32),
            pltpu.VMEM((24, elements), jnp.float32),
            pltpu.VMEM((SPLITS * 24, elements), jnp.float32),
            pltpu.VMEM((SPLITS * 48, 8 * elements), jnp.bfloat16),
        ],
        compiler_params=pltpu.CompilerParams(vmem_limit_bytes=24 * MIB),
        name="first_step" if first else "next_step",
    )(*args)


def final_kernel(modes, tiles, parts_ref, dense_ref, coords_ref, velocity_ref, external_ref,
                 coords_out, velocity_out, reduced_out, displaced_out, cols):
    coords, velocity, reduced = advance(parts_ref, coords_ref, velocity_ref, external_ref)
    coords_out[...] = coords
    velocity_out[...] = velocity
    reduced_out[...] = reduced
    cols[...] = column(coords)
    for i, row in enumerate(contract(owned_places(dense_ref, modes, tiles), cols, modes)):
        c, t = divmod(i, tiles)
        displaced_out[c, :, t * LANES : (t + 1) * LANES] = row


def finish(parts, dense, vectors):
    modes = vectors[0].shape[1]
    tiles = dense.shape[0] // (3 * modes)
    vector = jax.ShapeDtypeStruct((1, modes), jnp.float32)
    return pl.pallas_call(
        functools.partial(final_kernel, modes, tiles),
        out_shape=(vector, vector, vector, jax.ShapeDtypeStruct((3, 1, tiles * LANES), jnp.float32)),
        in_specs=[VMEM] * 5,
        out_specs=(VMEM,) * 4,
        scratch_shapes=[pltpu.VMEM((modes, LANES), jnp.float32)],
        compiler_params=pltpu.CompilerParams(vmem_limit_bytes=16 * MIB),
        name="finish",
    )(parts, dense, *vectors)


def exchange(below, above, axis):
    count = lax.axis_size(axis)
    up = [(i, (i + 1) % count) for i in range(count)]
    down = [(j, i) for i, j in up]
    from_above = lax.ppermute(below, axis, down)
    from_below = lax.ppermute(above, axis, up)
    return from_below, from_above


def everyone(parts, devices):
    chunks = parts.reshape(devices, parts.shape[0] // devices, LANES)
    return lax.all_to_all(chunks, ("gx", "gy"), 0, 0, tiled=True).reshape(parts.shape)


def shards(basis, connectivity, send_nodes, modulus, ecsw_weight, stiffness, coords, velocity, external):
    modes = coords.shape[0]
    nodes = basis.shape[3]
    flat = basis.reshape(3 * modes * nodes // LANES, LANES)
    links = connectivity[:, 0, :]
    coords, velocity, external = (x[None, :] for x in (coords, velocity, external))
    devices = lax.axis_size("gx") * lax.axis_size("gy")

    dense, pieces, hot, below, above = load(flat, send_nodes, modes)
    r2, r3 = exchange(below, above, "gy")
    below, above = share(pieces, hot, modes)
    r0, r1 = exchange(below, above, "gx")
    owned, low, high = prepare(dense, links, coords)
    sides = (r0, r1, r2, r3)

    (parts,) = step(True, owned, dense, sides, links, low, high, modulus, ecsw_weight, stiffness, (coords,), devices)
    for _ in range(STEPS - 1):
        parts, coords, velocity = step(
            False, everyone(parts, devices), dense, sides, links, low, high, modulus, ecsw_weight, stiffness,
            (coords, velocity, external), devices,
        )
    coords, velocity, reduced, displaced = finish(everyone(parts, devices), dense, (coords, velocity, external))
    return coords[0], velocity[0], reduced[0], displaced


def solution(mesh):
    return jax.shard_map(
        shards,
        mesh=mesh,
        in_specs=(
            P(None, None, "gx", "gy"),
            P(None, "gx", "gy"),
            P(None, "gx", "gy"),
            P("gx", "gy"),
            P("gx", "gy"),
            P(),
            P(),
            P(),
            P(),
        ),
        out_specs=(P(), P(), P(), P(None, "gx", "gy")),
        check_vma=False,
    )
```
